128 devices in a mesh: dom: 32 (over y, x, core), col: 4 (over z).
Axes of the slice: x: 4, y: 4, z: 4, core: 2. Of those that a mesh axis runs over, the one named last changes fastest.
Arguments:
- features: bfloat16 [262144, 1024], P('dom', 'col')
- weight: bfloat16 [1024, 1024], P(None, 'col'), may hold values from -0.1875 to 0.1875
- out_bias: bfloat16 [1024], P('col'), may hold values from -3 to 3
- local_index: int32 [32, 64, 4], P('dom'), may hold values from 0 to 63
- local_count: int32 [32, 64], P('dom'), may hold values from 1 to 4, as said below
- local_vals: bfloat16 [32, 64, 4, 128, 128], P('dom'), may hold values from -0.1875 to 0.1875
- halo_index: int32 [32, 64, 4], P('dom'), may hold values from 0 to 127
- halo_count: int32 [32, 64], P('dom'), may hold values from 0 to 4, as said below
- halo_vals: bfloat16 [32, 64, 4, 128, 128], P('dom'), may hold values from -0.1875 to 0.1875
- send_rows: int32 [32, 32, 512], P('dom'), may hold values from 0 to 8191
- send_count: int32 [32, 32], P('dom'), may hold values from 0 to 512, as said below
Outputs:
- normalized: bfloat16 [262144, 1024], P('dom', 'col')
- channel_stats: float32 [2, 1024], P(None, 'col')
The draws below stay inside these ranges and needn't reach their ends.
Inputs may be any that keep to these rules, and one draw needn't show every extreme that they name: `local_index`: slots k >= local_count of a row tile are not used. `local_count`: every partition has a row tile with all 4 slots used. `halo_index`: slots k >= halo_count of a row tile are not used. `halo_count`: every partition has a row tile with all 4 slots used. `send_rows`: slots s >= send_count[q, p] are not used. send_count[p, p] is 0; every partition fills all 512 slots to some other partition.
All inputs are finite; a program needn't handle non-finite values.
Results may differ from the reference program's by a relative error of at most 0.0075.
Values may be sent and summed in bfloat16 or wider, within the bound.
A program may use at most 192 MiB of HBM per device.

```python
import jax
import jax.numpy as jnp
from jax import lax

F = 1024
ROWS_DEV = 8192
TILE = 128
LOCAL_SLOTS = 4
HALO_SLOTS = 4
HALO_PEER = 512
NODES = 262144
LOCAL_TILES = 64
HALO_TILES = 128
N_DOM = 32


def draw_features(key, part):
    key_base = jax.random.fold_in(key, 0)
    rising = 1.0 + 2.0 * jnp.arange(NODES, dtype=jnp.float32) / NODES
    values = jax.random.normal(key_base, (NODES, F), jnp.float32) * rising[:, None]
    return values.astype(jnp.bfloat16)


def slot_counts(key, highest, lowest):
    key_base, key_heavy, key_place = jax.random.split(key, 3)
    counts = jax.random.randint(key_base, (N_DOM, LOCAL_TILES), lowest, highest + 1)
    heavier = jax.random.randint(key_heavy, (N_DOM, 1), 0, highest)
    counts = jnp.minimum(counts + heavier, highest)
    placed = jax.random.randint(key_place, (N_DOM, 1), 0, LOCAL_TILES)
    tile_ids = jnp.arange(LOCAL_TILES)[None, :]
    return jnp.where(tile_ids == placed, highest, counts).astype(jnp.int32)


def draw_local_count(key, part):
    return slot_counts(jax.random.fold_in(key, 11), LOCAL_SLOTS, 1)


def draw_halo_count(key, part):
    return slot_counts(jax.random.fold_in(key, 23), HALO_SLOTS, 0)


def draw_send_count(key, part):
    key_base, key_target = jax.random.split(jax.random.fold_in(key, 37))
    counts = jax.random.randint(key_base, (N_DOM, N_DOM), HALO_PEER // 4, HALO_PEER + 1)
    offset = jax.random.randint(key_target, (N_DOM, 1), 1, N_DOM)
    sources = jnp.arange(N_DOM)[:, None]
    targets = jnp.arange(N_DOM)[None, :]
    counts = jnp.where(targets == (sources + offset) % N_DOM, HALO_PEER, counts)
    return jnp.where(targets == sources, 0, counts).astype(jnp.int32)


def touch_ends(entries, key, low, high):
    longest = entries.shape.index(max(entries.shape))
    spots = []
    for shift in (0, 1):
        where = [jax.random.randint(jax.random.fold_in(key, axis), (), 0, length) for axis, length in enumerate(entries.shape)]
        where[longest] = (where[longest] + shift) % entries.shape[longest]
        spots.append(tuple(where))
    return entries.at[spots[0]].set(low).at[spots[1]].set(high)


def block_levels(stream_key, shape, cuts, least, high):
    level = 1.0
    for dim, shards_of in cuts:
        draws = jax.random.uniform(jax.random.fold_in(jax.random.fold_in(stream_key, 6), dim), (shards_of,), jnp.float32, least / len(cuts), high / len(cuts))
        level = level * jnp.repeat(jnp.exp(draws), shape[dim] // shards_of).reshape((-1,) + (1,) * (len(shape) - 1 - dim))
    return level


def bell_draw(stream_key, dims, deviation, reach, cuts=(), kind=jnp.bfloat16):
    entries = deviation * jax.random.normal(stream_key, dims, jnp.float32)
    if cuts:
        entries = entries * block_levels(stream_key, dims, cuts, -0.22, 0.18)
    return jnp.clip(entries, -reach, reach).astype(kind)


def setup_inputs(seed: int = 0) -> dict:
    arg_keys = jax.random.split(jax.random.key(seed), 12)
    features = draw_features(jax.random.fold_in(arg_keys[11], 71), 0)
    weight = bell_draw(arg_keys[1], (F, F), F ** -0.5, 0.1875, ((1, 4),))
    out_bias = bell_draw(arg_keys[2], (F,), 0.5, 3.0, ((0, 4),))
    local_index = touch_ends(jax.random.randint(arg_keys[3], (N_DOM, LOCAL_TILES, LOCAL_SLOTS), 0, LOCAL_TILES), jax.random.fold_in(arg_keys[3], 1), 0, LOCAL_TILES - 1).astype(jnp.int32)
    local_count = draw_local_count(jax.random.fold_in(arg_keys[11], 71), 0)
    local_vals = bell_draw(arg_keys[5], (N_DOM, LOCAL_TILES, LOCAL_SLOTS, TILE, TILE), (TILE * (LOCAL_SLOTS + HALO_SLOTS)) ** -0.5, 0.1875, ((0, 32),))
    halo_index = touch_ends(jax.random.randint(arg_keys[6], (N_DOM, LOCAL_TILES, HALO_SLOTS), 0, HALO_TILES), jax.random.fold_in(arg_keys[6], 1), 0, HALO_TILES - 1).astype(jnp.int32)
    halo_count = draw_halo_count(jax.random.fold_in(arg_keys[11], 71), 0)
    halo_vals = bell_draw(arg_keys[8], (N_DOM, LOCAL_TILES, HALO_SLOTS, TILE, TILE), (TILE * (LOCAL_SLOTS + HALO_SLOTS)) ** -0.5, 0.1875, ((0, 32),))
    send_rows = touch_ends(jax.random.randint(arg_keys[9], (N_DOM, N_DOM, HALO_PEER), 0, ROWS_DEV), jax.random.fold_in(arg_keys[9], 1), 0, ROWS_DEV - 1).astype(jnp.int32)
    send_count = draw_send_count(jax.random.fold_in(arg_keys[11], 71), 0)
    return {"features": features, "weight": weight, "out_bias": out_bias, "local_index": local_index, "local_count": local_count, "local_vals": local_vals, "halo_index": halo_index, "halo_count": halo_count, "halo_vals": halo_vals, "send_rows": send_rows, "send_count": send_count}


epsilon = 1e-06

def tile_product(sources, tile_index, tile_count, tile_vals, slot_total):
    gathered = sources[tile_index]
    keep_mask = jnp.arange(slot_total)[None, :] < tile_count[:, None]
    masked = jnp.where(keep_mask[:, :, None, None], tile_vals, jnp.zeros_like(tile_vals))
    return jnp.einsum('tkij,tkjc->tic', masked.astype(jnp.float32), gathered.astype(jnp.float32))

def reference(features, weight, out_bias, local_index, local_count, local_vals, halo_index, halo_count, halo_vals, send_rows, send_count):
    blocks = features.reshape(N_DOM, ROWS_DEV, F)
    slot_ids = jnp.arange(HALO_PEER)
    sources_ids = jnp.arange(N_DOM)

    def aggregate(partition):
        chosen = blocks[sources_ids[:, None], send_rows[:, partition, :]]
        keep_mask = slot_ids[None, :] < send_count[:, partition][:, None]
        halo_tiles = jnp.where(keep_mask[:, :, None], chosen, jnp.zeros_like(chosen)).reshape(HALO_TILES, TILE, F)
        own_tiles = blocks[partition].reshape(LOCAL_TILES, TILE, F)
        summed = tile_product(own_tiles, local_index[partition], local_count[partition], local_vals[partition], LOCAL_SLOTS)
        summed = summed + tile_product(halo_tiles, halo_index[partition], halo_count[partition], halo_vals[partition], HALO_SLOTS)
        return summed.reshape(ROWS_DEV, F).astype(jnp.bfloat16)
    spread = lax.map(aggregate, jnp.arange(N_DOM)).reshape(NODES, F)
    mixed_rows = jnp.dot(spread, weight, preferred_element_type=jnp.float32) + out_bias.astype(jnp.float32)
    active = jnp.maximum(mixed_rows, 0.0)
    row_power = lax.optimization_barrier(jnp.mean(active * active, axis=1, keepdims=True))
    scaled = active * lax.rsqrt(row_power + epsilon)
    channel_mean = lax.optimization_barrier(jnp.sum(scaled, axis=0)) / NODES
    channel_var = lax.optimization_barrier(jnp.sum(scaled * scaled, axis=0)) / NODES - channel_mean * channel_mean
    return (scaled.astype(jnp.bfloat16), jnp.stack([channel_mean, channel_var]))
```

```python
import functools

import jax
import jax.numpy as jnp
from jax import lax
from jax.experimental import pallas as pl
from jax.experimental.pallas import tpu as pltpu
from jax.sharding import PartitionSpec as P

MESH = pl.DeviceIdType.MESH
epsilon = 1e-06

T = 128
HALF = 256
UNROLL = 32
ZORD = (2, 1, 3)
CH = 256
SLOTS = 4


def dom_of(y, x, c):
    return (y * 4 + x) * 2 + c


def layer(
    sidx, lidx, hidx, feat_hbm, w_hbm, bias_hbm, lval, hval,
    out, stats,
    feat, tab, stage, send, mid, recv, acc, abuf, spread, zrecv, wbuf, bbuf, nbuf,
    part, zst, xst, yst, cst,
    in_sem, a_sem, w_send, w_recv, b_send, b_recv,
    mid_send, mid_recv, dir_send, fwd_send, fin_recv,
    z_send, z_recv, o_send, o_recv, own_sem,
    sz_send, sz_recv, sx_send, sx_recv, sy_send, sy_recv, sc_send, sc_recv,
):
    d = lax.axis_index("dom")
    z = lax.axis_index("col")
    y, x, c = d // 8, (d // 2) % 4, d % 2

    def place(r, du, dv):
        if isinstance(r, int):
            return ((y + dv) % 4, (x + du) % 4) if r == 0 else ((y + du) % 4, (x + dv) % 4)
        dy = jnp.where(r == 0, dv, du)
        dx = jnp.where(r == 0, du, dv)
        return (y + dy) % 4, (x + dx) % 4

    def remote(src, dst, ssem, rsem, dom, col):
        return pltpu.make_async_remote_copy(
            src_ref=src, dst_ref=dst, send_sem=ssem, recv_sem=rsem,
            device_id={"dom": dom, "col": col}, device_id_type=MESH,
        )

    barrier = pltpu.get_barrier_semaphore()
    peers = []
    for k in range(1, 4):
        for cc in range(2):
            peers.append((dom_of(y, (x + k) % 4, cc), z))
            peers.append((dom_of((y + k) % 4, x, cc), z))
        peers.append((d, (z + k) % 4))
    peers.append((dom_of(y, x, 1 - c), z))
    for dom, col in peers:
        pl.semaphore_signal(
            barrier, inc=1, device_id={"dom": dom, "col": col}, device_id_type=MESH
        )

    feat_in = pltpu.make_async_copy(feat_hbm, feat.at[pl.ds(0, 64)], in_sem.at[0])
    feat_in.start()
    w_in = pltpu.make_async_copy(w_hbm, wbuf.at[z], in_sem.at[1])
    w_in.start()
    b_in = pltpu.make_async_copy(bias_hbm, bbuf.at[z], in_sem.at[2])
    b_in.start()

    def a_chunk(vals, chunk, slot):
        return pltpu.make_async_copy(vals.at[pl.ds(chunk * 2, 2)], abuf.at[slot], a_sem.at[slot])

    for s in range(SLOTS):
        a_chunk(lval, s, s).start()

    row = lax.broadcasted_iota(jnp.int32, (256, 256), 0)
    lane = lax.broadcasted_iota(jnp.int32, (256, 256), 1)
    split = jnp.where(lane == 2 * (row % 128) + row // 128, 1.0, 0.0).astype(jnp.bfloat16)
    merge = jnp.where(row == 2 * (lane % 128) + lane // 128, 1.0, 0.0).astype(jnp.bfloat16)

    feat[64] = jnp.zeros((T, 256), jnp.bfloat16)
    tab[pl.ds(8192, 8)] = jnp.zeros((8, 2, 128), jnp.bfloat16)
    feat_in.wait()

    def build(i, carry):
        s = pl.ds(pl.multiple_of(i * T, T), T)
        rows = feat[i]
        both = jnp.concatenate([rows[:, :128], rows[:, 128:]], axis=0)
        mixed = jnp.dot(merge, both, preferred_element_type=jnp.float32).astype(jnp.bfloat16)
        tab[s] = mixed.reshape(T, 2, 128)
        return carry

    lax.fori_loop(0, 64, build, 0)
    w_in.wait()
    b_in.wait()
    pl.semaphore_wait(barrier, len(peers))

    def gather(dest, r, at):
        base = dest * 512 + r * HALF

        def rows(k, carry):
            for u in range(UNROLL):
                j = k * UNROLL + u
                stage[j] = tab[sidx[base + j]]
            return carry

        lax.fori_loop(0, HALF // UNROLL, rows, 0)
        for h in range(HALF // T):
            both = stage[pl.ds(h * T, T)].reshape(2 * T, 128)
            parts = jnp.dot(split, both, preferred_element_type=jnp.float32).astype(jnp.bfloat16)
            send[at + h, :, 0:128] = parts[:T]
            send[at + h, :, 128:256] = parts[T:]

    def mid_of(i):
        r = i % 2
        j = i // 2
        return r, 1 + j // 3, 1 + j % 3

    def mid_copy(i):
        r, du, dv = mid_of(i)
        ty, tx = place(r, du, 0)
        s = pl.ds(i * 4, 4)
        return remote(
            send.at[s], mid.at[s], mid_send.at[i], mid_recv.at[i], dom_of(ty, tx, c), z
        )

    def mid_step(i, carry):
        r, du, dv = mid_of(i)
        ty, tx = place(r, du, dv)
        for cc in range(2):
            gather(dom_of(ty, tx, (c + cc) % 2), r, i * 4 + cc * 2)
        mid_copy(i).start()
        return carry

    lax.fori_loop(0, 18, mid_step, 0)

    def dir_of(i):
        r = i % 2
        j = i // 2
        g = j // 6
        k = 1 + (j % 6) // 2
        cc = jnp.where(g == 2, 1, j % 2)
        du = jnp.where(g == 0, k, 0)
        dv = jnp.where(g == 1, k, 0)
        ty, tx = place(r, du, dv)
        return r, dom_of(ty, tx, (c + cc) % 2)

    def fin_slot(src, r):
        return pl.ds(src * 4 + r * 2, 2)

    def dir_copy(i):
        r, dest = dir_of(i)
        s = pl.ds(72 + i * 2, 2)
        return remote(
            send.at[s], recv.at[fin_slot(d, r)], dir_send.at[i], fin_recv.at[r * 32 + d], dest, z
        )

    def dir_step(i, carry):
        r, dest = dir_of(i)
        gather(dest, r, 72 + i * 2)
        dir_copy(i).start()
        return carry

    lax.fori_loop(0, 26, dir_step, 0)

    def w_copies(k):
        dst = (z + k) % 4
        return (
            remote(wbuf.at[z], wbuf.at[z], w_send.at[k - 1], w_recv.at[z], d, dst),
            remote(bbuf.at[z], bbuf.at[z], b_send.at[k - 1], b_recv.at[z], d, dst),
        )

    for k in range(1, 4):
        for cp in w_copies(k):
            cp.start()

    def fwd_copy(i, cc):
        r, du, dv = mid_of(i)
        ty, tx = place(r, 0, dv)
        sy, sx = place(r, 4 - du, 0)
        s = pl.ds(i * 4 + cc * 2, 2)
        src = dom_of(sy, sx, c)
        return remote(
            mid.at[s], recv.at[fin_slot(src, r)], fwd_send.at[i * 2 + cc],
            fin_recv.at[r * 32 + src], dom_of(ty, tx, (c + cc) % 2), z,
        )

    def fwd_step(i, carry):
        mid_copy(i).wait_recv()
        for cc in range(2):
            fwd_copy(i, cc).start()
        return carry

    lax.fori_loop(0, 18, fwd_step, 0)

    def tile_sum(slot, tt, idx, base, buf):
        total = None
        for k in (0, 2):
            lhs = jnp.concatenate([abuf[slot, tt, k], abuf[slot, tt, k + 1]], axis=1)
            rhs = jnp.concatenate(
                [buf[idx[base + k]], buf[idx[base + k + 1]]], axis=0
            )
            p = jnp.dot(lhs, rhs, preferred_element_type=jnp.float32)
            total = p if total is None else total + p
        return total

    def local_step(s, carry):
        slot = s % SLOTS
        a_chunk(lval, s, slot).wait()
        for tt in range(2):
            t = s * 2 + tt
            acc[pl.ds(pl.multiple_of(t * T, T), T), :] = tile_sum(slot, tt, lidx, t * 4, feat)

        @pl.when(s + SLOTS < 32)
        def _():
            a_chunk(lval, s + SLOTS, slot).start()

        return carry

    lax.fori_loop(0, 32, local_step, 0)

    def halo_chunk(s):
        q, o = s // 4, s % 4
        plane = (z + jnp.where(o == 0, ZORD[0], jnp.where(o == 1, ZORD[1], jnp.where(o == 2, ZORD[2], 0)))) % 4
        return q, o, plane

    def halo_vals(s, slot):
        q, o, plane = halo_chunk(s)
        return a_chunk(hval, plane * 8 + q, slot)

    for s in range(SLOTS):
        halo_vals(s, s).start()

    recv[pl.ds(d * 4, 4)] = jnp.zeros((4, T, 256), jnp.bfloat16)

    def fin_wait(src, r):
        remote(
            send.at[pl.ds(0, 2)], recv.at[fin_slot(src, r)], dir_send.at[0],
            fin_recv.at[r * 32 + src], d, z,
        ).wait_recv()

    def arrive(k, carry):
        src = (d + k) % 32
        for r in range(2):
            fin_wait(src, r)
        return carry

    lax.fori_loop(1, 32, arrive, 0)

    def z_copy(q, o, plane):
        s = pl.ds(pl.multiple_of(plane * 2048 + q * CH, CH), CH)
        return remote(
            spread.at[s], zrecv.at[z, pl.ds(pl.multiple_of(q * CH, CH), CH)],
            z_send.at[q * 3 + o], z_recv.at[q * 4 + z], d, plane,
        )

    def halo_step(s, carry):
        slot = s % SLOTS
        q, o, plane = halo_chunk(s)
        halo_vals(s, slot).wait()
        for tt in range(2):
            t = (plane * 8 + q) * 2 + tt
            rows = pl.ds(pl.multiple_of(t * T, T), T)
            total = acc[rows, :] + tile_sum(slot, tt, hidx, t * 4, recv)
            spread[rows, :] = total.astype(jnp.bfloat16)

        @pl.when(s + SLOTS < 32)
        def _():
            halo_vals(s + SLOTS, slot).start()

        @pl.when(o < 3)
        def _():
            z_copy(q, o, plane).start()

        return carry

    lax.fori_loop(0, 32, halo_step, 0)

    for k in range(1, 4):
        src = (z + k) % 4
        remote(wbuf.at[src], wbuf.at[src], w_send.at[0], w_recv.at[src], d, src).wait_recv()
        remote(bbuf.at[src], bbuf.at[src], b_send.at[0], b_recv.at[src], d, src).wait_recv()

    part[...] = jnp.zeros_like(part)

    def o_rows(plane, q):
        return pl.ds(pl.multiple_of(plane * 2048 + q * CH, CH), CH)

    def n_rows(q):
        return pl.ds(pl.multiple_of(q * CH, CH), CH)

    def o_copy(q, k):
        dst = (z + k) % 4
        return remote(
            nbuf.at[dst, n_rows(q)], out.at[o_rows(z, q)],
            o_send.at[q * 3 + k - 1], o_recv.at[q * 4 + z], d, dst,
        )

    def own_copy(q):
        return pltpu.make_async_copy(nbuf.at[z, n_rows(q)], out.at[o_rows(z, q)], own_sem.at[q])

    def z_wait(q, src):
        remote(
            spread.at[pl.ds(0, CH)], zrecv.at[src, n_rows(q)], z_send.at[0],
            z_recv.at[q * 4 + src], d, src,
        ).wait_recv()

    def mix_step(q, carry):
        zrecv[z, n_rows(q), :] = spread[o_rows(z, q), :]
        for k in range(1, 4):
            z_wait(q, (z + k) % 4)
        lhs = [zrecv[s, n_rows(q), :] for s in range(4)]
        acts = []
        power = None
        for b in range(4):
            total = None
            for s in range(4):
                p = jnp.dot(
                    lhs[s], wbuf[b, pl.ds(s * 256, 256), :], preferred_element_type=jnp.float32
                )
                total = p if total is None else total + p
            act = jnp.maximum(total + bbuf[b, 0:1, :].astype(jnp.float32), 0.0)
            acts.append(act)
            sq = jnp.sum(act * act, axis=1, keepdims=True)
            power = sq if power is None else power + sq
        scale = lax.rsqrt(power * (1.0 / 1024.0) + epsilon)
        for b in range(4):
            scaled = acts[b] * scale
            part[b, 0:1, :] += jnp.sum(scaled, axis=0, keepdims=True)
            part[b, 1:2, :] += jnp.sum(scaled * scaled, axis=0, keepdims=True)
            nbuf[b, n_rows(q), :] = scaled.astype(jnp.bfloat16)
        for k in (2, 1, 3):
            o_copy(q, k).start()
        own_copy(q).start()
        return carry

    lax.fori_loop(0, 8, mix_step, 0)

    zst[z] = part[z]
    for k in range(1, 4):
        dst = (z + k) % 4
        remote(part.at[dst], zst.at[z], sz_send.at[k - 1], sz_recv.at[z], d, dst).start()
    for k in range(1, 4):
        src = (z + k) % 4
        remote(part.at[src], zst.at[src], sz_send.at[0], sz_recv.at[src], d, src).wait_recv()
    xst[x] = zst[0] + zst[1] + zst[2] + zst[3]
    for k in range(1, 4):
        to = dom_of(y, (x + k) % 4, c)
        remote(xst.at[x], xst.at[x], sx_send.at[k - 1], sx_recv.at[x], to, z).start()
    for k in range(1, 4):
        src = (x + k) % 4
        remote(xst.at[src], xst.at[src], sx_send.at[0], sx_recv.at[src], d, z).wait_recv()
    yst[y] = xst[0] + xst[1] + xst[2] + xst[3]
    for k in range(1, 4):
        to = dom_of((y + k) % 4, x, c)
        remote(yst.at[y], yst.at[y], sy_send.at[k - 1], sy_recv.at[y], to, z).start()
    for k in range(1, 4):
        src = (y + k) % 4
        remote(yst.at[src], yst.at[src], sy_send.at[0], sy_recv.at[src], d, z).wait_recv()
    cst[c] = yst[0] + yst[1] + yst[2] + yst[3]
    other = dom_of(y, x, 1 - c)
    remote(cst.at[c], cst.at[c], sc_send.at[0], sc_recv.at[c], other, z).start()
    remote(cst.at[1 - c], cst.at[1 - c], sc_send.at[0], sc_recv.at[1 - c], other, z).wait_recv()
    sums = (cst[0] + cst[1]) * (1.0 / 262144.0)
    mean = sums[0:1, :]
    stats[0:1, :] = mean
    stats[1:2, :] = sums[1:2, :] - mean * mean

    def mid_done(i, carry):
        mid_copy(i).wait_send()
        for cc in range(2):
            fwd_copy(i, cc).wait_send()
        return carry

    lax.fori_loop(0, 18, mid_done, 0)

    def dir_done(i, carry):
        dir_copy(i).wait_send()
        return carry

    lax.fori_loop(0, 26, dir_done, 0)
    for k in range(1, 4):
        for cp in w_copies(k):
            cp.wait_send()
        dst = (z + k) % 4
        remote(part.at[dst], zst.at[z], sz_send.at[k - 1], sz_recv.at[z], d, dst).wait_send()
        to = dom_of(y, (x + k) % 4, c)
        remote(xst.at[x], xst.at[x], sx_send.at[k - 1], sx_recv.at[x], to, z).wait_send()
        to = dom_of((y + k) % 4, x, c)
        remote(yst.at[y], yst.at[y], sy_send.at[k - 1], sy_recv.at[y], to, z).wait_send()
    remote(cst.at[c], cst.at[c], sc_send.at[0], sc_recv.at[c], other, z).wait_send()

    def z_done(s, carry):
        q, o = s // 3, s % 3
        _, _, plane = halo_chunk(q * 4 + o)
        z_copy(q, o, plane).wait_send()
        return carry

    lax.fori_loop(0, 24, z_done, 0)

    def o_done(q, carry):
        own_copy(q).wait()
        for k in range(1, 4):
            o_copy(q, k).wait_send()
            src = (z + k) % 4
            remote(
                nbuf.at[0, n_rows(q)], out.at[o_rows(src, q)], o_send.at[0],
                o_recv.at[q * 4 + src], d, src,
            ).wait_recv()
        return carry

    lax.fori_loop(0, 8, o_done, 0)


def on_device(
    features, weight, out_bias, local_index, local_count, local_vals,
    halo_index, halo_count, halo_vals, send_rows, send_count,
):
    d = lax.axis_index("dom")
    slot = jnp.arange(512)[None, :]
    sidx = jnp.where(slot < send_count[0][:, None], send_rows[0], 8192).reshape(-1)
    four = jnp.arange(4)[None, :]
    lidx = jnp.where(four < local_count[0][:, None], local_index[0], 64).reshape(-1)
    hidx = jnp.where(four < halo_count[0][:, None], halo_index[0], d * 4).reshape(-1)
    bias = jnp.broadcast_to(out_bias[None, :], (16, 256))
    smem = pl.BlockSpec(memory_space=pltpu.SMEM)
    hbm = pl.BlockSpec(memory_space=pl.ANY)
    bf16, f32 = jnp.bfloat16, jnp.float32
    V = pltpu.VMEM
    dma = pltpu.SemaphoreType.DMA
    out, stats = pl.pallas_call(
        layer,
        out_shape=(
            jax.ShapeDtypeStruct((8192, 256), bf16),
            jax.ShapeDtypeStruct((2, 256), f32),
        ),
        in_specs=[smem, smem, smem, hbm, hbm, hbm, hbm, hbm],
        out_specs=(hbm, pl.BlockSpec(memory_space=V)),
        scratch_shapes=[
            V((65, T, 256), bf16),
            V((8192 + 8, 2, 128), bf16),
            V((HALF, 2, 128), bf16),
            V((72 + 26 * 2, T, 256), bf16),
            V((72, T, 256), bf16),
            V((128, T, 256), bf16),
            V((8192, 256), f32),
            V((SLOTS, 2, 4, 128, 128), bf16),
            V((8192, 256), bf16),
            V((4, 2048, 256), bf16),
            V((4, 1024, 256), bf16),
            V((4, 16, 256), bf16),
            V((4, 2048, 256), bf16),
            V((4, 8, 256), f32),
            V((4, 8, 256), f32),
            V((4, 8, 256), f32),
            V((4, 8, 256), f32),
            V((2, 8, 256), f32),
            dma((3,)), dma((SLOTS,)), dma((3,)), dma((4,)), dma((3,)), dma((4,)),
            dma((18,)), dma((18,)), dma((26,)), dma((36,)), dma((64,)),
            dma((24,)), dma((32,)), dma((24,)), dma((32,)), dma((8,)),
            dma((3,)), dma((4,)), dma((3,)), dma((4,)), dma((3,)), dma((4,)), dma((1,)), dma((2,)),
        ],
        compiler_params=pltpu.CompilerParams(
            collective_id=0, has_side_effects=True, vmem_limit_bytes=67043328
        ),
        name="layer",
    )(sidx, lidx, hidx, features.reshape(64, T, 256), weight, bias, local_vals[0], halo_vals[0])
    return out, stats


def solution(mesh):
    in_specs = (
        P("dom", "col"), P(None, "col"), P("col"),
        P("dom", None, None), P("dom", None), P("dom", None, None, None, None),
        P("dom", None, None), P("dom", None), P("dom", None, None, None, None),
        P("dom", None, None), P("dom", None),
    )
    return jax.shard_map(
        on_device, mesh=mesh, in_specs=in_specs,
        out_specs=(P("dom", "col"), P(None, "col")), check_vma=False,
    )
```

```python
import functools

import jax
import jax.numpy as jnp
from jax import lax
from jax.experimental import pallas as pl
from jax.experimental.pallas import tpu as pltpu
from jax.sharding import PartitionSpec as P

MESH = pl.DeviceIdType.MESH
epsilon = 1e-06

T = 128
HALF = 256
G = 64
ZORD = (2, 1, 3)
CH = 256
SLOTS = 4


def dom_of(y, x, c):
    return (y * 4 + x) * 2 + c


def layer(
    sidx, scnt, lidx, lcnt, hidx, hcnt, feat_hbm, w_hbm, bias_hbm, lval, hval,
    out, stats,
    feat, tab, stage, send, mid, recv, acc, abuf, spread, zrecv, wbuf, bbuf, nbuf,
    part, zst, xst, yst, cst,
    in_sem, a_sem, w_send, w_recv, b_send, b_recv,
    mid_send, mid_recv, dir_send, fwd_send, fin_recv,
    z_send, z_recv, o_send, o_recv, own_sem,
    sz_send, sz_recv, sx_send, sx_recv, sy_send, sy_recv, sc_send, sc_recv,
):
    d = lax.axis_index("dom")
    z = lax.axis_index("col")
    y, x, c = d // 8, (d // 2) % 4, d % 2

    def place(r, du, dv):
        if isinstance(r, int):
            return ((y + dv) % 4, (x + du) % 4) if r == 0 else ((y + du) % 4, (x + dv) % 4)
        dy = jnp.where(r == 0, dv, du)
        dx = jnp.where(r == 0, du, dv)
        return (y + dy) % 4, (x + dx) % 4

    def remote(src, dst, ssem, rsem, dom, col):
        return pltpu.make_async_remote_copy(
            src_ref=src, dst_ref=dst, send_sem=ssem, recv_sem=rsem,
            device_id={"dom": dom, "col": col}, device_id_type=MESH,
        )

    barrier = pltpu.get_barrier_semaphore()
    peers = []
    for k in range(1, 4):
        for cc in range(2):
            peers.append((dom_of(y, (x + k) % 4, cc), z))
            peers.append((dom_of((y + k) % 4, x, cc), z))
        peers.append((d, (z + k) % 4))
    peers.append((dom_of(y, x, 1 - c), z))
    for dom, col in peers:
        pl.semaphore_signal(
            barrier, inc=1, device_id={"dom": dom, "col": col}, device_id_type=MESH
        )

    feat_in = pltpu.make_async_copy(feat_hbm, feat.at[pl.ds(0, 64)], in_sem.at[0])
    feat_in.start()
    w_in = pltpu.make_async_copy(w_hbm, wbuf.at[z], in_sem.at[1])
    w_in.start()
    b_in = pltpu.make_async_copy(bias_hbm, bbuf.at[z], in_sem.at[2])
    b_in.start()

    def a_chunk(vals, chunk, slot):
        return pltpu.make_async_copy(vals.at[pl.ds(chunk * 2, 2)], abuf.at[slot], a_sem.at[slot])

    for s in range(SLOTS):
        a_chunk(lval, s, s).start()

    row = lax.broadcasted_iota(jnp.int32, (256, 256), 0)
    lane = lax.broadcasted_iota(jnp.int32, (256, 256), 1)
    srow = lax.broadcasted_iota(jnp.int32, (2 * G, 2 * G), 0)
    slane = lax.broadcasted_iota(jnp.int32, (2 * G, 2 * G), 1)
    split = jnp.where(slane == 2 * (srow % G) + srow // G, 1.0, 0.0).astype(jnp.bfloat16)
    merge = jnp.where(row == 2 * (lane % 128) + lane // 128, 1.0, 0.0).astype(jnp.bfloat16)

    feat[64] = jnp.zeros((T, 256), jnp.bfloat16)
    feat_in.wait()

    def build(i, carry):
        mixed = []
        for u in range(8):
            rows = feat[i * 8 + u]
            both = jnp.concatenate([rows[:, :128], rows[:, 128:]], axis=0)
            mixed.append(jnp.dot(merge, both, preferred_element_type=jnp.float32).astype(jnp.bfloat16))
        for u in range(8):
            s = pl.ds(pl.multiple_of(i * 1024 + u * T, T), T)
            tab[s] = mixed[u].reshape(T, 2, 128)
        return carry

    lax.fori_loop(0, 8, build, 0)
    w_in.wait()
    b_in.wait()
    pl.semaphore_wait(barrier, len(peers))

    row_id = lax.broadcasted_iota(jnp.int32, (G, 128), 0)

    def gather(dest, r, at):
        used = scnt[0, dest] - r * HALF
        for g in range(HALF // G):
            for u in range(G):
                stage[g * G + u] = tab[sidx[dest, r * HALF + g * G + u]]
            both = stage[pl.ds(g * G, G)].reshape(2 * G, 128)
            parts = jnp.dot(split, both, preferred_element_type=jnp.float32)
            keep = row_id < used - g * G
            rows = pl.ds(g * G % T, G)
            for h in range(2):
                half = jnp.where(keep, parts[h * G : (h + 1) * G], 0.0)
                send[at + g * G // T, rows, h * 128 : (h + 1) * 128] = half.astype(jnp.bfloat16)

    def mid_of(i):
        r = i % 2
        j = i // 2
        return r, 1 + (j * 2) % 3, 1 + j // 3

    def mid_copy(i):
        r, du, dv = mid_of(i)
        ty, tx = place(r, du, 0)
        s = pl.ds(i * 4, 4)
        return remote(
            send.at[s], mid.at[s], mid_send.at[i], mid_recv.at[i], dom_of(ty, tx, c), z
        )

    def mid_step(i, carry):
        r, du, dv = mid_of(i)
        ty, tx = place(r, du, dv)
        for cc in range(2):
            gather(dom_of(ty, tx, (c + cc) % 2), r, i * 4 + cc * 2)
        mid_copy(i).start()
        return carry

    lax.fori_loop(0, 18, mid_step, 0)

    def dir_of(i):
        r = i % 2
        j = i // 2
        g = j // 6
        k = 1 + (j % 6) // 2
        cc = jnp.where(g == 2, 1, j % 2)
        du = jnp.where(g == 0, k, 0)
        dv = jnp.where(g == 1, k, 0)
        ty, tx = place(r, du, dv)
        return r, dom_of(ty, tx, (c + cc) % 2)

    def fin_slot(src, r):
        return pl.ds(src * 4 + r * 2, 2)

    def dir_copy(i):
        r, dest = dir_of(i)
        s = pl.ds(72 + i * 2, 2)
        return remote(
            send.at[s], recv.at[fin_slot(d, r)], dir_send.at[i], fin_recv.at[r * 32 + d], dest, z
        )

    def fwd_copy(i, cc):
        r, du, dv = mid_of(i)
        ty, tx = place(r, 0, dv)
        sy, sx = place(r, 4 - du, 0)
        s = pl.ds(i * 4 + cc * 2, 2)
        src = dom_of(sy, sx, c)
        return remote(
            mid.at[s], recv.at[fin_slot(src, r)], fwd_send.at[i * 2 + cc],
            fin_recv.at[r * 32 + src], dom_of(ty, tx, (c + cc) % 2), z,
        )

    def fwd_step(i):
        mid_copy(i).wait_recv()
        for cc in range(2):
            fwd_copy(i, cc).start()

    def dir_step(i, carry):
        r, dest = dir_of(i)
        gather(dest, r, 72 + i * 2)
        dir_copy(i).start()

        @pl.when(i < 18)
        def _():
            fwd_step(i)

        return carry

    lax.fori_loop(0, 26, dir_step, 0)

    def w_copies(k):
        dst = (z + k) % 4
        return (
            remote(wbuf.at[z], wbuf.at[z], w_send.at[k - 1], w_recv.at[z], d, dst),
            remote(bbuf.at[z], bbuf.at[z], b_send.at[k - 1], b_recv.at[z], d, dst),
        )

    for k in range(1, 4):
        for cp in w_copies(k):
            cp.start()

    def tile_sum(slot, tt, idx, cnt, zero, t, buf):
        total = None
        at = [jnp.where(k < cnt[0, t], idx[k, t], zero) for k in range(4)]
        for k in (0, 2):
            lhs = jnp.concatenate([abuf[slot, tt, k], abuf[slot, tt, k + 1]], axis=1)
            rhs = jnp.concatenate(
                [buf[at[k]], buf[at[k + 1]]], axis=0
            )
            p = jnp.dot(lhs, rhs, preferred_element_type=jnp.float32)
            total = p if total is None else total + p
        return total

    def local_step(s, carry):
        slot = s % SLOTS
        a_chunk(lval, s, slot).wait()
        for tt in range(2):
            t = s * 2 + tt
            acc[pl.ds(pl.multiple_of(t * T, T), T), :] = tile_sum(slot, tt, lidx, lcnt, 64, t, feat)

        @pl.when(s + SLOTS < 32)
        def _():
            a_chunk(lval, s + SLOTS, slot).start()

        return carry

    lax.fori_loop(0, 32, local_step, 0)

    def halo_chunk(s):
        q, o = s // 4, s % 4
        plane = (z + jnp.where(o == 0, ZORD[0], jnp.where(o == 1, ZORD[1], jnp.where(o == 2, ZORD[2], 0)))) % 4
        return q, o, plane

    def halo_vals(s, slot):
        q, o, plane = halo_chunk(s)
        return a_chunk(hval, plane * 8 + q, slot)

    for s in range(SLOTS):
        halo_vals(s, s).start()

    recv[pl.ds(d * 4, 4)] = jnp.zeros((4, T, 256), jnp.bfloat16)

    def fin_wait(src, r):
        remote(
            send.at[pl.ds(0, 2)], recv.at[fin_slot(src, r)], dir_send.at[0],
            fin_recv.at[r * 32 + src], d, z,
        ).wait_recv()

    def arrive(k, carry):
        src = (d + k) % 32
        for r in range(2):
            fin_wait(src, r)
        return carry

    lax.fori_loop(1, 32, arrive, 0)

    def z_copy(q, o, plane):
        s = pl.ds(pl.multiple_of(plane * 2048 + q * CH, CH), CH)
        return remote(
            spread.at[s], zrecv.at[z, pl.ds(pl.multiple_of(q * CH, CH), CH)],
            z_send.at[q * 3 + o], z_recv.at[q * 4 + z], d, plane,
        )

    def halo_step(s, carry):
        slot = s % SLOTS
        q, o, plane = halo_chunk(s)
        halo_vals(s, slot).wait()
        for tt in range(2):
            t = (plane * 8 + q) * 2 + tt
            rows = pl.ds(pl.multiple_of(t * T, T), T)
            total = acc[rows, :] + tile_sum(slot, tt, hidx, hcnt, d * 4, t, recv)
            spread[rows, :] = total.astype(jnp.bfloat16)

        @pl.when(s + SLOTS < 32)
        def _():
            halo_vals(s + SLOTS, slot).start()

        @pl.when(o < 3)
        def _():
            z_copy(q, o, plane).start()

        return carry

    lax.fori_loop(0, 32, halo_step, 0)

    for k in range(1, 4):
        src = (z + k) % 4
        remote(wbuf.at[src], wbuf.at[src], w_send.at[0], w_recv.at[src], d, src).wait_recv()
        remote(bbuf.at[src], bbuf.at[src], b_send.at[0], b_recv.at[src], d, src).wait_recv()

    part[...] = jnp.zeros_like(part)

    def o_rows(plane, q):
        return pl.ds(pl.multiple_of(plane * 2048 + q * CH, CH), CH)

    def n_rows(q):
        return pl.ds(pl.multiple_of(q * CH, CH), CH)

    def o_copy(q, k):
        dst = (z + k) % 4
        return remote(
            nbuf.at[dst, n_rows(q)], out.at[o_rows(z, q)],
            o_send.at[q * 3 + k - 1], o_recv.at[q * 4 + z], d, dst,
        )

    def own_copy(q):
        return pltpu.make_async_copy(nbuf.at[z, n_rows(q)], out.at[o_rows(z, q)], own_sem.at[q])

    def z_wait(q, src):
        remote(
            spread.at[pl.ds(0, CH)], zrecv.at[src, n_rows(q)], z_send.at[0],
            z_recv.at[q * 4 + src], d, src,
        ).wait_recv()

    def mix_step(q, carry):
        zrecv[z, n_rows(q), :] = spread[o_rows(z, q), :]
        for k in range(1, 4):
            z_wait(q, (z + k) % 4)
        lhs = [zrecv[s, n_rows(q), :] for s in range(4)]
        acts = []
        power = None
        for b in range(4):
            total = None
            for s in range(4):
                p = jnp.dot(
                    lhs[s], wbuf[b, pl.ds(s * 256, 256), :], preferred_element_type=jnp.float32
                )
                total = p if total is None else total + p
            act = jnp.maximum(total + bbuf[b].astype(jnp.float32), 0.0)
            acts.append(act)
            sq = jnp.sum(act * act, axis=1, keepdims=True)
            power = sq if power is None else power + sq
        scale = lax.rsqrt(power * (1.0 / 1024.0) + epsilon)
        for b in range(4):
            scaled = acts[b] * scale
            part[b, 0:1, :] += jnp.sum(scaled, axis=0, keepdims=True)
            part[b, 1:2, :] += jnp.sum(scaled * scaled, axis=0, keepdims=True)
            nbuf[b, n_rows(q), :] = scaled.astype(jnp.bfloat16)
        for k in (2, 1, 3):
            o_copy(q, k).start()
        own_copy(q).start()
        return carry

    lax.fori_loop(0, 8, mix_step, 0)

    def x_sum(k):
        to = dom_of(y, (x + k) % 4, c)
        return remote(xst.at[x], xst.at[x], sx_send.at[k - 1], sx_recv.at[x], to, z)

    def y_sum(k):
        to = dom_of((y + k) % 4, x, c)
        return remote(yst.at[y], yst.at[y], sy_send.at[k - 1], sy_recv.at[y], to, z)

    def c_sum():
        to = dom_of(y, x, 1 - c)
        return remote(cst.at[c], cst.at[c], sc_send.at[0], sc_recv.at[c], to, z)

    def z_sum(k):
        dst = (z + k) % 4
        return remote(part.at[dst], zst.at[z], sz_send.at[k - 1], sz_recv.at[z], d, dst)

    xst[x] = part[...]
    for k in range(1, 4):
        x_sum(k).start()
    for k in range(1, 4):
        src = (x + k) % 4
        remote(xst.at[src], xst.at[src], sx_send.at[0], sx_recv.at[src], d, z).wait_recv()
    yst[y] = xst[0] + xst[1] + xst[2] + xst[3]
    for k in range(1, 4):
        y_sum(k).start()
    for k in range(1, 4):
        src = (y + k) % 4
        remote(yst.at[src], yst.at[src], sy_send.at[0], sy_recv.at[src], d, z).wait_recv()
    cst[c] = yst[0] + yst[1] + yst[2] + yst[3]
    c_sum().start()
    remote(cst.at[1 - c], cst.at[1 - c], sc_send.at[0], sc_recv.at[1 - c], d, z).wait_recv()
    part[...] = cst[0] + cst[1]
    zst[z] = part[z]
    for k in range(1, 4):
        z_sum(k).start()

    def mid_done(i, carry):
        mid_copy(i).wait_send()
        for cc in range(2):
            fwd_copy(i, cc).wait_send()
        return carry

    lax.fori_loop(0, 18, mid_done, 0)

    def dir_done(i, carry):
        dir_copy(i).wait_send()
        return carry

    lax.fori_loop(0, 26, dir_done, 0)
    for k in range(1, 4):
        for cp in w_copies(k):
            cp.wait_send()
        x_sum(k).wait_send()
        y_sum(k).wait_send()
    c_sum().wait_send()

    def z_done(s, carry):
        q, o = s // 3, s % 3
        _, _, plane = halo_chunk(q * 4 + o)
        z_copy(q, o, plane).wait_send()
        return carry

    lax.fori_loop(0, 24, z_done, 0)

    def o_done(q, carry):
        own_copy(q).wait()
        for k in range(1, 4):
            o_copy(q, k).wait_send()
            src = (z + k) % 4
            remote(
                nbuf.at[0, n_rows(q)], out.at[o_rows(src, q)], o_send.at[0],
                o_recv.at[q * 4 + src], d, src,
            ).wait_recv()
        return carry

    lax.fori_loop(0, 8, o_done, 0)

    for k in range(1, 4):
        src = (z + k) % 4
        remote(part.at[src], zst.at[src], sz_send.at[0], sz_recv.at[src], d, src).wait_recv()
        z_sum(k).wait_send()
    sums = (zst[0] + zst[1] + zst[2] + zst[3]) * (1.0 / 262144.0)
    mean = sums[0:1, :]
    stats[0:1, :] = mean
    stats[1:2, :] = sums[1:2, :] - mean * mean


def on_device(
    features, weight, out_bias, local_index, local_count, local_vals,
    halo_index, halo_count, halo_vals, send_rows, send_count,
):
    smem = pl.BlockSpec(memory_space=pltpu.SMEM)
    hbm = pl.BlockSpec(memory_space=pl.ANY)
    bf16, f32 = jnp.bfloat16, jnp.float32
    V = pltpu.VMEM
    dma = pltpu.SemaphoreType.DMA
    out, stats = pl.pallas_call(
        layer,
        out_shape=(
            jax.ShapeDtypeStruct((8192, 256), bf16),
            jax.ShapeDtypeStruct((2, 256), f32),
        ),
        in_specs=[smem] * 6 + [hbm, hbm, hbm, hbm, hbm],
        out_specs=(hbm, pl.BlockSpec(memory_space=V)),
        scratch_shapes=[
            V((65, T, 256), bf16),
            V((8192, 2, 128), bf16),
            V((HALF, 2, 128), bf16),
            V((72 + 26 * 2, T, 256), bf16),
            V((72, T, 256), bf16),
            V((128, T, 256), bf16),
            V((8192, 256), f32),
            V((SLOTS, 2, 4, 128, 128), bf16),
            V((8192, 256), bf16),
            V((4, 2048, 256), bf16),
            V((4, 1024, 256), bf16),
            V((4, 1, 256), bf16),
            V((4, 2048, 256), bf16),
            V((4, 2, 256), f32),
            V((4, 2, 256), f32),
            V((4, 4, 2, 256), f32),
            V((4, 4, 2, 256), f32),
            V((2, 4, 2, 256), f32),
            dma((3,)), dma((SLOTS,)), dma((3,)), dma((4,)), dma((3,)), dma((4,)),
            dma((18,)), dma((18,)), dma((26,)), dma((36,)), dma((64,)),
            dma((24,)), dma((32,)), dma((24,)), dma((32,)), dma((8,)),
            dma((3,)), dma((4,)), dma((3,)), dma((4,)), dma((3,)), dma((4,)), dma((1,)), dma((2,)),
        ],
        compiler_params=pltpu.CompilerParams(
            collective_id=0, has_side_effects=True, vmem_limit_bytes=67043328
        ),
        name="layer",
    )(
        send_rows[0], send_count, local_index[0].T, local_count, halo_index[0].T, halo_count,
        features.reshape(64, T, 256), weight, out_bias.reshape(1, 256), local_vals[0], halo_vals[0],
    )
    return out, stats


def solution(mesh):
    in_specs = (
        P("dom", "col"), P(None, "col"), P("col"),
        P("dom", None, None), P("dom", None), P("dom", None, None, None, None),
        P("dom", None, None), P("dom", None), P("dom", None, None, None, None),
        P("dom", None, None), P("dom", None),
    )
    return jax.shard_map(
        on_device, mesh=mesh, in_specs=in_specs,
        out_specs=(P("dom", "col"), P(None, "col")), check_vma=False,
    )
```

```python
import jax
import jax.numpy as jnp
from jax import lax
from jax.experimental import pallas as pl
from jax.experimental.pallas import tpu as pltpu
from jax.sharding import PartitionSpec as P

MESH = pl.DeviceIdType.MESH
epsilon = 1e-06

T = 128
HALF = 256
G = 64
ZORD = (2, 1, 3)
SPLIT = 12
SLOTS = 4
N = 128


def dom_of(y, x, c):
    return (y * 4 + x) * 2 + c


def layer(
    sidx, scnt, lidx, lcnt, hidx, hcnt, feat_hbm, w_hbm, bias_hbm, lval, hval,
    out, stats,
    feat, tab, stage, send, mid, mid2, recv, recv2, acc, abuf, zrecv, wbuf, bbuf, nbuf,
    zb, ya, pa, pb, part, s1, s2,
    in_sem, a_sem, w_send, w_recv, wg_send, wg_recv, b_send, b_recv,
    mid_send, mid_recv, mid_recv2, dir_send, fwd_send, fin_recv, fin_recv2,
    z_send, z_recv, z_recv2, n_send, zb_recv, o_recv, pa_send, pa_recv, pb_send, pb_recv,
    s1_send, s1_recv, s2_send, s2_recv,
):
    f32, bf16 = jnp.float32, jnp.bfloat16
    d = lax.axis_index("dom")
    z = lax.axis_index("col")
    y, x, c = d // 8, (d // 2) % 4, d % 2

    def place(r, du, dv):
        dy = jnp.where(r == 0, dv, du)
        dx = jnp.where(r == 0, du, dv)
        return (y + dy) % 4, (x + dx) % 4

    def remote(src, dst, ssem, rsem, dom, col):
        return pltpu.make_async_remote_copy(
            src_ref=src, dst_ref=dst, send_sem=ssem, recv_sem=rsem,
            device_id={"dom": dom, "col": col}, device_id_type=MESH,
        )

    barrier = pltpu.get_barrier_semaphore()
    peers = []
    for k in range(1, 4):
        for cc in range(2):
            peers.append((dom_of(y, (x + k) % 4, cc), z))
            peers.append((dom_of((y + k) % 4, x, cc), z))
        peers.append((d, (z + k) % 4))
    peers.append((dom_of(y, x, 1 - c), z))
    for dom, col in peers:
        pl.semaphore_signal(
            barrier, inc=1, device_id={"dom": dom, "col": col}, device_id_type=MESH
        )

    feat_in = pltpu.make_async_copy(feat_hbm, feat.at[pl.ds(0, 64)], in_sem.at[0])
    feat_in.start()
    w_in = pltpu.make_async_copy(w_hbm, wbuf.at[z], in_sem.at[1])
    w_in.start()
    b_in = pltpu.make_async_copy(bias_hbm, bbuf.at[z], in_sem.at[2])
    b_in.start()

    def a_chunk(vals, chunk, slot):
        return pltpu.make_async_copy(vals.at[pl.ds(chunk * 2, 2)], abuf.at[slot], a_sem.at[slot])

    for s in range(SLOTS):
        a_chunk(lval, s, s).start()

    row = lax.broadcasted_iota(jnp.int32, (256, 256), 0)
    lane = lax.broadcasted_iota(jnp.int32, (256, 256), 1)
    merge = jnp.where(row == 2 * (lane % 128) + lane // 128, 1.0, 0.0).astype(bf16)
    srow = lax.broadcasted_iota(jnp.int32, (2 * G, 2 * G), 0)
    slane = lax.broadcasted_iota(jnp.int32, (2 * G, 2 * G), 1)
    split = jnp.where(slane == 2 * (srow % G) + srow // G, 1.0, 0.0).astype(bf16)
    row_id = lax.broadcasted_iota(jnp.int32, (G, 128), 0)
    lane_id = lax.broadcasted_iota(jnp.int32, (G, 128), 1)

    feat[64] = jnp.zeros((T, 256), bf16)
    zb[64] = jnp.zeros((T, N), bf16)
    feat_in.wait()

    def build(i, carry):
        mixed = []
        for u in range(8):
            rows = feat[i * 8 + u]
            both = jnp.concatenate([rows[:, :128], rows[:, 128:]], axis=0)
            mixed.append(jnp.dot(merge, both, preferred_element_type=f32).astype(bf16))
        for u in range(8):
            tab[pl.ds(pl.multiple_of(i * 1024 + u * T, T), T)] = mixed[u].reshape(T, 2, 128)
        return carry

    lax.fori_loop(0, 8, build, 0)
    w_in.wait()
    b_in.wait()
    pl.semaphore_wait(barrier, len(peers))

    other = dom_of(y, x, 1 - c)

    def w_part(plane, h, core):
        return wbuf.at[plane, pl.ds(core * 512, 512), pl.ds(h * N, N)]

    def w_copy(k, h):
        part = w_part(z, h, c)
        return remote(part, part, w_send.at[h * 3 + k - 1], w_recv.at[h * 4 + z], d, (z + k) % 4)

    def w_give(k, h):
        src = (z + k) % 4
        part = w_part(src, h, c)
        return remote(part, part, wg_send.at[h * 3 + k - 1], wg_recv.at[h * 4 + src], other, z)

    def bias_copy(k):
        return remote(bbuf.at[z], bbuf.at[z], b_send.at[k - 1], b_recv.at[z], d, (z + k) % 4)

    def w_wait(h):
        for k in range(1, 4):
            src = (z + k) % 4
            part = w_part(src, h, c)
            remote(part, part, w_send.at[0], w_recv.at[h * 4 + src], d, src).wait_recv()
            w_give(k, h).start()
        for k in range(1, 4):
            src = (z + k) % 4
            part = w_part(src, h, 1 - c)
            remote(part, part, wg_send.at[0], wg_recv.at[h * 4 + src], d, z).wait_recv()

    for k in range(1, 4):
        w_copy(k, 1).start()

    def z_plane(o):
        far = jnp.where(o == 0, ZORD[0], jnp.where(o == 1, ZORD[1], jnp.where(o == 2, ZORD[2], 0)))
        return (z + far) % 4

    def z_copy(q, o, sems):
        plane = z_plane(o)
        return remote(
            feat.at[pl.ds(plane * 16 + q * 2, 2)], zrecv.at[z, pl.ds(q * 2, 2)],
            z_send.at[q * 3 + o], sems.at[q * 4 + z], d, plane,
        )

    def z_first(s, carry):
        z_copy(s // 3, s % 3, z_recv).start()
        return carry

    lax.fori_loop(0, 24, z_first, 0)

    def gather(dest, r, at, narrow):
        used = scnt[0, dest] - r * HALF
        base = dest * 512 + r * HALF
        for g in range(HALF // G):
            for u in range(G):
                stage[g * G + u] = tab[sidx[base + (g * G + u)]]
            both = stage[pl.ds(g * G, G)].reshape(2 * G, 128)
            parts = jnp.dot(split, both, preferred_element_type=f32)
            keep = row_id < used - g * G
            rows = pl.ds(g * G % T, G)
            if narrow:
                whole = jnp.where(lane_id < 64, parts[:G], pltpu.roll(parts[G:], 64, 1))
                send[at + g * G // T, rows, 0:128] = jnp.where(keep, whole, 0.0).astype(bf16)
            else:
                for h in range(2):
                    half = jnp.where(keep, parts[h * G : (h + 1) * G], 0.0)
                    send[at + g * G // T, rows, h * 128 : (h + 1) * 128] = half.astype(bf16)

    def mid_of(i):
        r = i % 2
        j = i // 2
        return r, 1 + (j * 2) % 3, 1 + j // 3

    def sent(at, n, narrow):
        return send.at[pl.ds(at, n), :, pl.ds(0, 128)] if narrow else send.at[pl.ds(at, n)]

    def mid_copy(i, narrow):
        r, du, dv = mid_of(i)
        ty, tx = place(r, du, 0)
        buf, sems = (mid2, mid_recv2) if narrow else (mid, mid_recv)
        return remote(
            sent(i * 4, 4, narrow), buf.at[pl.ds(i * 4, 4)], mid_send.at[i], sems.at[i],
            dom_of(ty, tx, c), z,
        )

    def mid_step(i, narrow):
        r, du, dv = mid_of(i)
        ty, tx = place(r, du, dv)

        def core(cc, carry):
            gather(dom_of(ty, tx, (c + cc) % 2), r, i * 4 + cc * 2, narrow)
            return carry

        lax.fori_loop(0, 2, core, 0)
        mid_copy(i, narrow).start()

    def dir_of(i):
        r = i % 2
        j = i // 2
        g = j // 6
        k = 1 + (j % 6) // 2
        cc = jnp.where(g == 2, 1, j % 2)
        du = jnp.where(g == 0, k, 0)
        dv = jnp.where(g == 1, k, 0)
        ty, tx = place(r, du, dv)
        return r, dom_of(ty, tx, (c + cc) % 2)

    def fin_at(src, r, narrow):
        buf, sems = (recv2, fin_recv2) if narrow else (recv, fin_recv)
        return buf.at[pl.ds(src * 4 + r * 2, 2)], sems.at[r * 32 + src]

    def dir_copy(i, narrow):
        r, dest = dir_of(i)
        dst, sem = fin_at(d, r, narrow)
        return remote(sent(72 + i * 2, 2, narrow), dst, dir_send.at[i], sem, dest, z)

    def fwd_copy(i, cc, narrow):
        r, du, dv = mid_of(i)
        ty, tx = place(r, 0, dv)
        sy, sx = place(r, 4 - du, 0)
        dst, sem = fin_at(dom_of(sy, sx, c), r, narrow)
        buf = mid2 if narrow else mid
        return remote(
            buf.at[pl.ds(i * 4 + cc * 2, 2)], dst, fwd_send.at[i * 2 + cc], sem,
            dom_of(ty, tx, (c + cc) % 2), z,
        )

    def dir_step(i, narrow):
        r, dest = dir_of(i)
        gather(dest, r, 72 + i * 2, narrow)
        dir_copy(i, narrow).start()

        @pl.when(i < 18)
        def _():
            mid_copy(i, narrow).wait_recv()
            for cc in range(2):
                fwd_copy(i, cc, narrow).start()

    def first_mid(i, carry):
        mid_step(i, False)
        return carry

    lax.fori_loop(0, 18, first_mid, 0)

    def two(q):
        return pl.ds(q * 2, 2)

    def mine(q):
        return pl.ds(z * 16 + q * 2, 2)

    def z_wait(q, src, sems):
        remote(
            feat.at[pl.ds(0, 2)], zrecv.at[src, two(q)], z_send.at[0],
            sems.at[q * 4 + src], d, src,
        ).wait_recv()

    def mix(q, sems, col):
        zrecv[z, two(q)] = feat[mine(q)]
        for k in range(1, 4):
            z_wait(q, (z + k) % 4, sems)
        lhs = [zrecv[s, two(q)].reshape(256, 256) for s in range(4)]
        res = []
        for b in (0, 2):
            total = None
            for s in range(4):
                w = [wbuf[b + e, s * 256 : (s + 1) * 256, col : col + N] for e in range(2)]
                p = jnp.dot(lhs[s], jnp.concatenate(w, axis=1), preferred_element_type=f32)
                total = p if total is None else total + p
            res.append(total)
        return res

    def back_copy(q, k, buf, sems):
        dst = (z + k) % 4
        return remote(
            nbuf.at[dst, two(q)], buf.at[mine(q)], n_send.at[q * 3 + k - 1],
            sems.at[q * 4 + z], d, dst,
        )

    def back_wait(q, src, buf, sems):
        remote(
            nbuf.at[0, two(q)], buf.at[pl.ds(src * 16 + q * 2, 2)], n_send.at[0],
            sems.at[q * 4 + src], d, src,
        ).wait_recv()

    def premix_step(q, carry):
        res = mix(q, z_recv, N)
        for b in range(4):
            half = res[b // 2][:, (b % 2) * N : (b % 2 + 1) * N]
            nbuf[b, two(q)] = half.astype(bf16).reshape(2, T, N)
        for k in ZORD:
            back_copy(q, k, zb, zb_recv).start()
        zb[mine(q)] = nbuf[z, two(q)]
        return carry

    def first_dir(i, carry):
        dir_step(i, False)

        @pl.when(i % 5 == 3)
        def _():
            premix_step(i // 5, 0)

        return carry

    w_wait(1)
    lax.fori_loop(0, 26, first_dir, 0)
    lax.fori_loop(5, 6, premix_step, 0)

    def tile_sum(slot, tt, idx, cnt, zero, t, buf):
        total = None
        at = [jnp.where(k < cnt[0, t], idx[k, t], zero) for k in range(4)]
        for k in (0, 2):
            lhs = jnp.concatenate([abuf[slot, tt, k], abuf[slot, tt, k + 1]], axis=1)
            rhs = jnp.concatenate([buf[at[k]], buf[at[k + 1]]], axis=0)
            p = jnp.dot(lhs, rhs, preferred_element_type=f32)
            total = p if total is None else total + p
        return total

    def stream(vals, chunk_of, use):
        def step(s, carry):
            slot = s % SLOTS
            a_chunk(vals, chunk_of(s), slot).wait()
            use(s, slot)

            @pl.when(s + SLOTS < 32)
            def _():
                a_chunk(vals, chunk_of(s + SLOTS), slot).start()

            return carry

        lax.fori_loop(0, 32, step, 0)

    def ahead(vals, chunk_of):
        for s in range(SLOTS):
            a_chunk(vals, chunk_of(s), s).start()

    def t_rows(t):
        return pl.ds(pl.multiple_of(t * T, T), T)

    def in_order(s):
        return s

    def own_a(s, slot):
        for tt in range(2):
            t = s * 2 + tt
            acc[t_rows(t), :] = tile_sum(slot, tt, lidx, lcnt, 64, t, feat)

    stream(lval, in_order, own_a)
    lax.fori_loop(6, 8, premix_step, 0)
    for k in range(1, 4):
        w_copy(k, 0).start()
        bias_copy(k).start()

    def halo_chunk(s):
        return z_plane(s % 4) * 8 + s // 4

    ahead(hval, halo_chunk)

    def zb_wait(q, carry):
        for k in range(1, 4):
            back_wait(q, (z + k) % 4, zb, zb_recv)
        return carry

    lax.fori_loop(0, 8, zb_wait, 0)

    def rebuild(i, carry):
        mixed = []
        for u in range(8):
            rows = zb[i * 8 + u]
            turned = pltpu.roll(rows.astype(f32), 64, 1).astype(bf16)
            both = jnp.concatenate([rows, turned], axis=0)
            mixed.append(jnp.dot(merge, both, preferred_element_type=f32).astype(bf16))
        for u in range(8):
            tab[pl.ds(pl.multiple_of(i * 1024 + u * T, T), T)] = mixed[u].reshape(T, 2, 128)
        return carry

    lax.fori_loop(0, 8, rebuild, 0)

    def second_mid(i, carry):
        mid_copy(i, False).wait_send()
        mid_step(i, True)
        return carry

    lax.fori_loop(0, SPLIT, second_mid, 0)

    recv[pl.ds(d * 4, 4)] = jnp.zeros((4, T, 256), bf16)
    recv2[pl.ds(d * 4, 4)] = jnp.zeros((4, T, N), bf16)

    def z_sent(s, carry):
        z_copy(s // 3, s % 3, z_recv).wait_send()
        return carry

    lax.fori_loop(0, 24, z_sent, 0)

    def arrive(k, narrow):
        src = (d + k) % 32
        for r in range(2):
            dst, sem = fin_at(src, r, narrow)
            remote(sent(0, 2, narrow), dst, dir_send.at[0], sem, d, z).wait_recv()

    def first_arrive(k, carry):
        arrive(k, False)
        return carry

    lax.fori_loop(1, 32, first_arrive, 0)

    def halo_a(s, slot):
        chunk = halo_chunk(s)
        for tt in range(2):
            t = chunk * 2 + tt
            total = acc[t_rows(t), :] + tile_sum(slot, tt, hidx, hcnt, d * 4, t, recv)
            feat[t] = total.astype(bf16)

        @pl.when(s % 4 < 3)
        def _():
            z_copy(s // 4, s % 4, z_recv2).start()

    stream(hval, halo_chunk, halo_a)
    ahead(lval, in_order)

    lax.fori_loop(SPLIT, 18, second_mid, 0)

    def first_sent(i, carry):
        for cc in range(2):
            fwd_copy(i, cc, False).wait_send()
        return carry

    lax.fori_loop(0, 18, first_sent, 0)

    def second_dir(i, carry):
        dir_copy(i, False).wait_send()
        dir_step(i, True)
        return carry

    lax.fori_loop(0, 26, second_dir, 0)

    def own_b(s, slot):
        for tt in range(2):
            t = s * 2 + tt
            acc[t_rows(t), 0:N] = tile_sum(slot, tt, lidx, lcnt, 64, t, zb)

    stream(lval, in_order, own_b)
    ahead(hval, in_order)

    def back_sent(q, carry):
        for k in range(1, 4):
            back_copy(q, k, zb, zb_recv).wait_send()
        return carry

    lax.fori_loop(0, 8, back_sent, 0)

    def as_row(col):
        return jnp.broadcast_to(col, (256, 128)).T[0:1, :]

    def pa_copy(q, k):
        dst = (z + k) % 4
        return remote(
            pa.at[z, q], pa.at[z, q], pa_send.at[q * 3 + k - 1], pa_recv.at[q * 4 + z], d, dst
        )

    def mix_step(q, carry):
        res = mix(q, z_recv2, 0)
        power = None
        for b in (0, 2):
            bias = jnp.concatenate([bbuf[b], bbuf[b + 1]], axis=1)
            keep = jnp.concatenate([bias[:, 0:N], bias[:, 256 : 256 + N]], axis=1)
            act = jnp.maximum(res[b // 2] + keep.astype(f32), 0.0)
            p = jnp.sum(act * act, axis=1, keepdims=True)
            power = p if power is None else power + p
            for e in range(2):
                half = act[:, e * N : (e + 1) * N]
                nbuf[b + e, two(q)] = half.astype(bf16).reshape(2, T, N)
        pa[z, q] = as_row(power)
        for k in ZORD:
            back_copy(q, k, ya, o_recv).start()
            pa_copy(q, k).start()
        ya[mine(q)] = nbuf[z, two(q)]
        return carry

    w_wait(0)
    for k in range(1, 4):
        src = (z + k) % 4
        remote(bbuf.at[src], bbuf.at[src], b_send.at[0], b_recv.at[src], d, src).wait_recv()
    lax.fori_loop(0, 8, mix_step, 0)

    def second_arrive(k, carry):
        arrive(k, True)
        return carry

    lax.fori_loop(1, 32, second_arrive, 0)

    def halo_b(s, slot):
        power = []
        for tt in range(2):
            t = s * 2 + tt
            total = acc[t_rows(t), 0:N] + tile_sum(slot, tt, hidx, hcnt, d * 4, t, recv2)
            act = jnp.maximum(total + bbuf[z][:, N : 2 * N].astype(f32), 0.0)
            acc[t_rows(t), 0:N] = act
            power.append(jnp.sum(act * act, axis=1, keepdims=True))
        pb[z, s] = as_row(jnp.concatenate(power, axis=0))

    stream(hval, in_order, halo_b)

    def pb_copy(k):
        return remote(pb.at[z], pb.at[z], pb_send.at[k - 1], pb_recv.at[z], d, (z + k) % 4)

    for k in range(1, 4):
        pb_copy(k).start()
    for k in range(1, 4):
        src = (z + k) % 4
        remote(pb.at[src], pb.at[src], pb_send.at[0], pb_recv.at[src], d, src).wait_recv()

    part[...] = jnp.zeros_like(part)

    def norm_step(q, carry):
        for k in range(1, 4):
            src = (z + k) % 4
            back_wait(q, src, ya, o_recv)
            remote(pa.at[src, q], pa.at[src, q], pa_send.at[0], pa_recv.at[q * 4 + src], d, src).wait_recv()
        sums = [[None, None], [None, None]]
        for p in range(4):
            chunk = p * 8 + q
            power = pa[p, q] + pb[0, chunk] + pb[1, chunk] + pb[2, chunk] + pb[3, chunk]
            scale = jnp.broadcast_to(lax.rsqrt(power * (1.0 / 1024.0) + epsilon), (128, 256)).T
            at = pl.ds(p * 16 + q * 2, 2)
            acts = (
                ya[at].reshape(256, N).astype(f32),
                acc[pl.ds(pl.multiple_of(chunk * 256, 256), 256), 0:N],
            )
            for h in range(2):
                scaled = acts[h] * scale
                out[at, :, h * N : (h + 1) * N] = scaled.astype(bf16).reshape(2, T, N)
                for e, v in enumerate((scaled, scaled * scaled)):
                    v = jnp.sum(v, axis=0, keepdims=True)
                    sums[h][e] = v if sums[h][e] is None else sums[h][e] + v
        for h in range(2):
            for e in range(2):
                part[e : e + 1, h * N : (h + 1) * N] += sums[h][e]
        return carry

    lax.fori_loop(0, 8, norm_step, 0)

    me = x * 2 + c

    def s1_copy(k):
        to = (me + k) % 8
        return remote(s1.at[me], s1.at[me], s1_send.at[k - 1], s1_recv.at[me], y * 8 + to, z)

    def s2_copy(k):
        to = dom_of((y + k) % 4, x, c)
        return remote(s2.at[y], s2.at[y], s2_send.at[k - 1], s2_recv.at[y], to, z)

    s1[me] = part[...]
    for k in range(1, 8):
        s1_copy(k).start()
    for k in range(1, 8):
        src = (me + k) % 8
        remote(s1.at[src], s1.at[src], s1_send.at[0], s1_recv.at[src], d, z).wait_recv()
    total = s1[0]
    for k in range(1, 8):
        total = total + s1[k]
    s2[y] = total
    for k in range(1, 4):
        s2_copy(k).start()

    def last_mid(i, carry):
        mid_copy(i, True).wait_send()
        for cc in range(2):
            fwd_copy(i, cc, True).wait_send()
        return carry

    lax.fori_loop(0, 18, last_mid, 0)

    def last_dir(i, carry):
        dir_copy(i, True).wait_send()
        return carry

    lax.fori_loop(0, 26, last_dir, 0)

    def last_z(s, carry):
        z_copy(s // 3, s % 3, z_recv2).wait_send()
        return carry

    lax.fori_loop(0, 24, last_z, 0)

    def last_back(q, carry):
        for k in range(1, 4):
            back_copy(q, k, ya, o_recv).wait_send()
            pa_copy(q, k).wait_send()
        return carry

    lax.fori_loop(0, 8, last_back, 0)
    for k in range(1, 4):
        for h in range(2):
            w_copy(k, h).wait_send()
            w_give(k, h).wait_send()
        bias_copy(k).wait_send()
        pb_copy(k).wait_send()
    for k in range(1, 8):
        s1_copy(k).wait_send()
    for k in range(1, 4):
        src = (y + k) % 4
        remote(s2.at[src], s2.at[src], s2_send.at[0], s2_recv.at[src], d, z).wait_recv()
        s2_copy(k).wait_send()
    sums = (s2[0] + s2[1] + s2[2] + s2[3]) * (1.0 / 262144.0)
    mean = sums[0:1, :]
    stats[0:1, :] = mean
    stats[1:2, :] = sums[1:2, :] - mean * mean


def on_device(
    features, weight, out_bias, local_index, local_count, local_vals,
    halo_index, halo_count, halo_vals, send_rows, send_count,
):
    smem = pl.BlockSpec(memory_space=pltpu.SMEM)
    hbm = pl.BlockSpec(memory_space=pl.ANY)
    bf16, f32 = jnp.bfloat16, jnp.float32
    V = pltpu.VMEM
    dma = lambda n: pltpu.SemaphoreType.DMA((n,))
    out, stats = pl.pallas_call(
        layer,
        out_shape=(V((64, T, 256), bf16), V((2, 256), f32)),
        in_specs=[smem] * 6 + [hbm] * 5,
        out_specs=(pl.BlockSpec(memory_space=V), pl.BlockSpec(memory_space=V)),
        scratch_shapes=[
            V((65, T, 256), bf16),
            V((8192, 2, 128), bf16),
            V((HALF, 2, 128), bf16),
            V((72 + 26 * 2, T, 256), bf16),
            V((72, T, 256), bf16),
            V((72, T, N), bf16),
            V((128, T, 256), bf16),
            V((128, T, N), bf16),
            V((8192, 256), f32),
            V((SLOTS, 2, 4, 128, 128), bf16),
            V((4, 16, T, 256), bf16),
            V((4, 1024, 256), bf16),
            V((4, 1, 256), bf16),
            V((4, 16, T, N), bf16),
            V((65, T, N), bf16),
            V((64, T, N), bf16),
            V((4, 8, 1, 256), f32),
            V((4, 32, 1, 256), f32),
            V((2, 256), f32),
            V((8, 2, 256), f32),
            V((4, 2, 256), f32),
            dma(3), dma(SLOTS), dma(6), dma(8), dma(6), dma(8), dma(3), dma(4),
            dma(18), dma(18), dma(18), dma(26), dma(36), dma(64), dma(64),
            dma(24), dma(32), dma(32), dma(24), dma(32), dma(32), dma(24), dma(32), dma(3), dma(4),
            dma(7), dma(8), dma(3), dma(4),
        ],
        compiler_params=pltpu.CompilerParams(
            collective_id=0, has_side_effects=True, vmem_limit_bytes=62000000
        ),
        name="layer",
    )(
        send_rows.reshape(-1), send_count, local_index[0].T, local_count, halo_index[0].T, halo_count,
        features.reshape(64, T, 256), weight, out_bias.reshape(1, 256), local_vals[0], halo_vals[0],
    )
    return out.reshape(8192, 256), stats


def solution(mesh):
    in_specs = (
        P("dom", "col"), P(None, "col"), P("col"),
        P("dom", None, None), P("dom", None), P("dom", None, None, None, None),
        P("dom", None, None), P("dom", None), P("dom", None, None, None, None),
        P("dom", None, None), P("dom", None),
    )
    return jax.shard_map(
        on_device, mesh=mesh, in_specs=in_specs,
        out_specs=(P("dom", "col"), P(None, "col")), check_vma=False,
    )
```

```python
import jax
import jax.numpy as jnp
from jax import lax
from jax.experimental import pallas as pl
from jax.experimental.pallas import tpu as pltpu
from jax.sharding import PartitionSpec as P

MESH = pl.DeviceIdType.MESH
epsilon = 1e-06

T = 128
HALF = 256
G = 64
ZORD = (2, 1, 3)
LATE = 6
SPLIT = 12
SLOTS = 4
N = 128


def dom_of(y, x, c):
    return (y * 4 + x) * 2 + c


def layer(
    sidx_hbm, scnt, lidx, lcnt, hidx, hcnt, feat_hbm, w_hbm, bias_hbm, lval, hval,
    out, stats,
    sidx, feat, tab, stage, send, mid, mid2, recv, recv2, acc, abuf, zrecv, wbuf, bbuf, b_own, nbuf,
    zb, ya, pa, pb, part, s1,
    in_sem, idx_sem, a_sem, w_send, w_recv, wg_send, wg_recv, b_send, b_recv,
    mid_send, mid_recv, mid_recv2, dir_send, fwd_send, fin_recv, fin_recv2,
    z_send, z_recv, z_recv2, n_send, zb_recv, o_recv, pa_send, pa_recv, pb_send, pb_recv,
    s1_send, s1_recv,
):
    f32, bf16 = jnp.float32, jnp.bfloat16
    d = lax.axis_index("dom")
    z = lax.axis_index("col")
    y, x, c = d // 8, (d // 2) % 4, d % 2

    def place(r, du, dv):
        dy = jnp.where(r == 0, dv, du)
        dx = jnp.where(r == 0, du, dv)
        return (y + dy) % 4, (x + dx) % 4

    def remote(src, dst, ssem, rsem, dom, col):
        return pltpu.make_async_remote_copy(
            src_ref=src, dst_ref=dst, send_sem=ssem, recv_sem=rsem,
            device_id={"dom": dom, "col": col}, device_id_type=MESH,
        )

    def feat_in(i):
        tiles = pl.ds(i * 8, 8)
        return pltpu.make_async_copy(feat_hbm.at[tiles], feat.at[tiles], in_sem.at[4 + i])

    for i in range(8):
        feat_in(i).start()

    def idx_in(p):
        return pltpu.make_async_copy(sidx_hbm.at[p], sidx.at[pl.ds(p * 512, 512)], idx_sem.at[p])

    for p in range(32):
        idx_in(p).start()
    w_in = pltpu.make_async_copy(w_hbm, wbuf.at[z], in_sem.at[1])
    w_in.start()
    b_in = pltpu.make_async_copy(bias_hbm, b_own, in_sem.at[2])
    b_in.start()

    def a_chunk(vals, chunk, slot):
        return pltpu.make_async_copy(vals.at[pl.ds(chunk * 2, 2)], abuf.at[slot], a_sem.at[slot])

    for s in range(SLOTS):
        a_chunk(lval, s, s).start()

    barrier = pltpu.get_barrier_semaphore()
    peers = [((d + k) % 32, z) for k in range(1, 32)] + [(d, (z + k) % 4) for k in range(1, 4)]
    for dom, col in peers:
        pl.semaphore_signal(
            barrier, inc=1, device_id={"dom": dom, "col": col}, device_id_type=MESH
        )


    row = lax.broadcasted_iota(jnp.int32, (256, 256), 0)
    lane = lax.broadcasted_iota(jnp.int32, (256, 256), 1)
    merge = jnp.where(row == 2 * (lane % 128) + lane // 128, 1.0, 0.0).astype(bf16)
    srow = lax.broadcasted_iota(jnp.int32, (2 * G, 2 * G), 0)
    slane = lax.broadcasted_iota(jnp.int32, (2 * G, 2 * G), 1)
    split = jnp.where(slane == 2 * (srow % G) + srow // G, 1.0, 0.0).astype(bf16)
    row_id = lax.broadcasted_iota(jnp.int32, (G, 128), 0)
    lane_id = lax.broadcasted_iota(jnp.int32, (G, 128), 1)

    feat[64] = jnp.zeros((T, 256), bf16)
    zb[64] = jnp.zeros((T, N), bf16)
    def build(i, carry):
        feat_in(i).wait()
        mixed = []
        for u in range(0, 8, 2):
            rows = [feat[i * 8 + u + e] for e in range(2)]
            both = jnp.concatenate(
                [
                    jnp.concatenate([rows[0][:, :128], rows[1][:, :128]], axis=1),
                    jnp.concatenate([rows[0][:, 128:], rows[1][:, 128:]], axis=1),
                ],
                axis=0,
            )
            mixed.append(jnp.dot(merge, both, preferred_element_type=f32).astype(bf16))
        for u in range(8):
            half = mixed[u // 2][:, u % 2 * 128 : (u % 2 + 1) * 128]
            tab[pl.ds(pl.multiple_of(i * 1024 + u * T, T), T)] = half.reshape(T, 2, 128)
        return carry

    lax.fori_loop(0, 8, build, 0)
    w_in.wait()
    b_in.wait()
    bbuf[z] = b_own[...].reshape(1, 256)
    for p in range(32):
        idx_in(p).wait()
    pl.semaphore_wait(barrier, len(peers))

    other = dom_of(y, x, 1 - c)

    def w_part(plane, h, core):
        return wbuf.at[plane, pl.ds(core * 512, 512), pl.ds(h * N, N)]

    def w_copy(k, h):
        part = w_part(z, h, c)
        return remote(part, part, w_send.at[h * 3 + k - 1], w_recv.at[h * 4 + z], d, (z + k) % 4)

    def w_give(k, h):
        src = (z + k) % 4
        part = w_part(src, h, c)
        return remote(part, part, wg_send.at[h * 3 + k - 1], wg_recv.at[h * 4 + src], other, z)

    def bias_copy(k):
        return remote(bbuf.at[z], bbuf.at[z], b_send.at[k - 1], b_recv.at[z], d, (z + k) % 4)

    def w_wait(h):
        for k in range(1, 4):
            src = (z + k) % 4
            part = w_part(src, h, c)
            remote(part, part, w_send.at[0], w_recv.at[h * 4 + src], d, src).wait_recv()
            w_give(k, h).start()
        for k in range(1, 4):
            src = (z + k) % 4
            part = w_part(src, h, 1 - c)
            remote(part, part, wg_send.at[0], wg_recv.at[h * 4 + src], d, z).wait_recv()

    for k in range(1, 4):
        w_copy(k, 1).start()

    def z_plane(o):
        far = jnp.where(o == 0, ZORD[0], jnp.where(o == 1, ZORD[1], jnp.where(o == 2, ZORD[2], 0)))
        return (z + far) % 4

    def z_copy(q, o, sems):
        plane = z_plane(o)
        return remote(
            feat.at[pl.ds(plane * 16 + q * 2, 2)], zrecv.at[z, pl.ds(q * 2, 2)],
            z_send.at[q * 3 + o], sems.at[q * 4 + z], d, plane,
        )

    def z_first(s, carry):
        z_copy(s // 3, s % 3, z_recv).start()
        return carry

    lax.fori_loop(0, 24, z_first, 0)

    def gather(dest, r, at, narrow):
        used = scnt[0, dest] - r * HALF
        base = dest * 512 + r * HALF
        for g in range(HALF // G):
            for u in range(G):
                stage[g * G + u] = tab[sidx[base + (g * G + u)]]
            both = stage[pl.ds(g * G, G)].reshape(2 * G, 128)
            parts = jnp.dot(split, both, preferred_element_type=f32)
            keep = row_id < used - g * G
            rows = pl.ds(g * G % T, G)
            if narrow:
                whole = jnp.where(lane_id < 64, parts[:G], pltpu.roll(parts[G:], 64, 1))
                send[at + g * G // T, rows, 0:128] = jnp.where(keep, whole, 0.0).astype(bf16)
            else:
                for h in range(2):
                    half = jnp.where(keep, parts[h * G : (h + 1) * G], 0.0)
                    send[at + g * G // T, rows, h * 128 : (h + 1) * 128] = half.astype(bf16)

    def mid_of(i):
        r = i % 2
        j = i // 2
        return r, 1 + (j * 2) % 3, 1 + j // 3

    def sent(at, n, narrow):
        return send.at[pl.ds(at, n), :, pl.ds(0, 128)] if narrow else send.at[pl.ds(at, n)]

    def mid_copy(i, narrow):
        r, du, dv = mid_of(i)
        ty, tx = place(r, du, 0)
        buf, sems = (mid2, mid_recv2) if narrow else (mid, mid_recv)
        return remote(
            sent(i * 4, 4, narrow), buf.at[pl.ds(i * 4, 4)], mid_send.at[i], sems.at[i],
            dom_of(ty, tx, c), z,
        )

    def mid_step(i, narrow):
        r, du, dv = mid_of(i)
        ty, tx = place(r, du, dv)

        def core(cc, carry):
            gather(dom_of(ty, tx, (c + cc) % 2), r, i * 4 + cc * 2, narrow)
            return carry

        lax.fori_loop(0, 2, core, 0)
        mid_copy(i, narrow).start()

    def dir_of(i):
        r = i % 2
        j = i // 2
        g = j // 6
        k = 1 + (j % 6) // 2
        cc = jnp.where(g == 2, 1, j % 2)
        du = jnp.where(g == 0, k, 0)
        dv = jnp.where(g == 1, k, 0)
        ty, tx = place(r, du, dv)
        return r, dom_of(ty, tx, (c + cc) % 2)

    def fin_at(src, r, narrow):
        buf, sems = (recv2, fin_recv2) if narrow else (recv, fin_recv)
        return buf.at[pl.ds(src * 4 + r * 2, 2)], sems.at[r * 32 + src]

    def dir_copy(i, narrow):
        r, dest = dir_of(i)
        dst, sem = fin_at(d, r, narrow)
        return remote(sent(72 + i * 2, 2, narrow), dst, dir_send.at[i], sem, dest, z)

    def fwd_copy(i, cc, narrow):
        r, du, dv = mid_of(i)
        ty, tx = place(r, 0, dv)
        sy, sx = place(r, 4 - du, 0)
        dst, sem = fin_at(dom_of(sy, sx, c), r, narrow)
        buf = mid2 if narrow else mid
        return remote(
            buf.at[pl.ds(i * 4 + cc * 2, 2)], dst, fwd_send.at[i * 2 + cc], sem,
            dom_of(ty, tx, (c + cc) % 2), z,
        )

    def dir_step(i, narrow):
        r, dest = dir_of(i)
        gather(dest, r, 72 + i * 2, narrow)
        dir_copy(i, narrow).start()

        @pl.when(i < 18)
        def _():
            mid_copy(i, narrow).wait_recv()
            for cc in range(2):
                fwd_copy(i, cc, narrow).start()

    def first_mid(i, carry):
        mid_step(i, False)
        return carry

    lax.fori_loop(0, 18, first_mid, 0)

    def two(q):
        return pl.ds(q * 2, 2)

    def mine(q):
        return pl.ds(z * 16 + q * 2, 2)

    def z_wait(q, src, sems):
        remote(
            feat.at[pl.ds(0, 2)], zrecv.at[src, two(q)], z_send.at[0],
            sems.at[q * 4 + src], d, src,
        ).wait_recv()

    def mix(q, sems, col):
        zrecv[z, two(q)] = feat[mine(q)]
        for k in range(1, 4):
            z_wait(q, (z + k) % 4, sems)
        lhs = [zrecv[s, two(q)].reshape(256, 256) for s in range(4)]
        res = []
        for b in (0, 2):
            total = None
            for s in range(4):
                w = [wbuf[b + e, s * 256 : (s + 1) * 256, col : col + N] for e in range(2)]
                p = jnp.dot(lhs[s], jnp.concatenate(w, axis=1), preferred_element_type=f32)
                total = p if total is None else total + p
            res.append(total)
        return res

    def back_copy(q, k, buf, sems):
        dst = (z + k) % 4
        return remote(
            nbuf.at[dst, two(q)], buf.at[mine(q)], n_send.at[q * 3 + k - 1],
            sems.at[q * 4 + z], d, dst,
        )

    def back_wait(q, src, buf, sems):
        remote(
            nbuf.at[0, two(q)], buf.at[pl.ds(src * 16 + q * 2, 2)], n_send.at[0],
            sems.at[q * 4 + src], d, src,
        ).wait_recv()

    def premix_step(q, carry):
        res = mix(q, z_recv, N)
        for b in range(4):
            half = res[b // 2][:, (b % 2) * N : (b % 2 + 1) * N]
            nbuf[b, two(q)] = half.astype(bf16).reshape(2, T, N)
        for k in ZORD:
            back_copy(q, k, zb, zb_recv).start()
        zb[mine(q)] = nbuf[z, two(q)]
        return carry

    def first_dir(i, carry):
        dir_step(i, False)

        @pl.when(i % 5 == 4)
        def _():
            premix_step(i // 5, 0)

        return carry

    lax.fori_loop(0, 3, first_dir, 0)
    w_wait(1)
    lax.fori_loop(3, 26, first_dir, 0)
    lax.fori_loop(5, 6, premix_step, 0)

    def tile_sum(slot, tt, idx, cnt, zero, t, buf):
        total = None
        at = [jnp.where(k < cnt[0, t], idx[k, t], zero) for k in range(4)]
        for k in (0, 2):
            lhs = jnp.concatenate([abuf[slot, tt, k], abuf[slot, tt, k + 1]], axis=1)
            rhs = jnp.concatenate([buf[at[k]], buf[at[k + 1]]], axis=0)
            p = jnp.dot(lhs, rhs, preferred_element_type=f32)
            total = p if total is None else total + p
        return total

    def stream(vals, chunk_of, use):
        def step(s, carry):
            slot = s % SLOTS
            a_chunk(vals, chunk_of(s), slot).wait()
            use(s, slot)

            @pl.when(s + SLOTS < 32)
            def _():
                a_chunk(vals, chunk_of(s + SLOTS), slot).start()

            return carry

        lax.fori_loop(0, 32, step, 0)

    def ahead(vals, chunk_of):
        for s in range(SLOTS):
            a_chunk(vals, chunk_of(s), s).start()

    def t_rows(t):
        return pl.ds(pl.multiple_of(t * T, T), T)

    def in_order(s):
        return s

    def own_a(s, slot):
        for tt in range(2):
            t = s * 2 + tt
            acc[t_rows(t), :] = tile_sum(slot, tt, lidx, lcnt, 64, t, feat)

    stream(lval, in_order, own_a)
    lax.fori_loop(6, 8, premix_step, 0)
    for k in range(1, 4):
        w_copy(k, 0).start()
        bias_copy(k).start()

    def halo_chunk(s):
        return z_plane(s % 4) * 8 + s // 4

    ahead(hval, halo_chunk)

    def zb_wait(q, carry):
        for k in range(1, 4):
            back_wait(q, (z + k) % 4, zb, zb_recv)
        return carry

    lax.fori_loop(0, 8, zb_wait, 0)

    def rebuild(i, carry):
        mixed = []
        for u in range(0, 8, 2):
            rows = jnp.concatenate([zb[i * 8 + u], zb[i * 8 + u + 1]], axis=1)
            turned = [pltpu.roll(zb[i * 8 + u + e].astype(f32), 64, 1).astype(bf16) for e in range(2)]
            both = jnp.concatenate([rows, jnp.concatenate(turned, axis=1)], axis=0)
            mixed.append(jnp.dot(merge, both, preferred_element_type=f32).astype(bf16))
        for u in range(8):
            half = mixed[u // 2][:, u % 2 * 128 : (u % 2 + 1) * 128]
            tab[pl.ds(pl.multiple_of(i * 1024 + u * T, T), T)] = half.reshape(T, 2, 128)
        return carry

    lax.fori_loop(0, 8, rebuild, 0)

    def second_mid(i, carry):
        mid_copy(i, False).wait_send()
        mid_step(i, True)
        return carry

    lax.fori_loop(0, SPLIT, second_mid, 0)

    recv[pl.ds(d * 4, 4)] = jnp.zeros((4, T, 256), bf16)
    recv2[pl.ds(d * 4, 4)] = jnp.zeros((4, T, N), bf16)

    def z_sent(s, carry):
        z_copy(s // 3, s % 3, z_recv).wait_send()
        return carry

    lax.fori_loop(0, 24, z_sent, 0)

    def arrive(k, narrow):
        src = (d + k) % 32
        for r in range(2):
            dst, sem = fin_at(src, r, narrow)
            remote(sent(0, 2, narrow), dst, dir_send.at[0], sem, d, z).wait_recv()

    def first_arrive(k, carry):
        arrive(k, False)
        return carry

    lax.fori_loop(1, 32, first_arrive, 0)

    def halo_a(s, slot):
        chunk = halo_chunk(s)
        for tt in range(2):
            t = chunk * 2 + tt
            total = acc[t_rows(t), :] + tile_sum(slot, tt, hidx, hcnt, d * 4, t, recv)
            feat[t] = total.astype(bf16)

        @pl.when(s % 4 < 3)
        def _():
            z_copy(s // 4, s % 4, z_recv2).start()

    stream(hval, halo_chunk, halo_a)
    ahead(lval, in_order)

    lax.fori_loop(SPLIT, 18, second_mid, 0)

    def first_sent(i, carry):
        for cc in range(2):
            fwd_copy(i, cc, False).wait_send()
        return carry

    lax.fori_loop(0, 18, first_sent, 0)

    def second_dir(i, carry):
        dir_copy(i, False).wait_send()
        dir_step(i, True)
        return carry

    lax.fori_loop(0, 26, second_dir, 0)

    def own_b(s, slot):
        for tt in range(2):
            t = s * 2 + tt
            acc[t_rows(t), 0:N] = tile_sum(slot, tt, lidx, lcnt, 64, t, zb)

    stream(lval, in_order, own_b)
    ahead(hval, in_order)

    def back_sent(q, carry):
        for k in range(1, 4):
            back_copy(q, k, zb, zb_recv).wait_send()
        return carry

    lax.fori_loop(0, 8, back_sent, 0)

    def power_row(square):
        return jnp.sum(square.T, axis=0, keepdims=True)

    def pa_copy(q, k):
        dst = (z + k) % 4
        return remote(
            pa.at[z, q], pa.at[z, q], pa_send.at[q * 3 + k - 1], pa_recv.at[q * 4 + z], d, dst
        )

    def mix_step(q, carry):
        res = mix(q, z_recv2, 0)
        power = None
        for b in (0, 2):
            bias = jnp.concatenate([bbuf[b], bbuf[b + 1]], axis=1)
            keep = jnp.concatenate([bias[:, 0:N], bias[:, 256 : 256 + N]], axis=1)
            act = jnp.maximum(res[b // 2] + keep.astype(f32), 0.0)
            for e in range(2):
                half = act[:, e * N : (e + 1) * N]
                p = half * half
                power = p if power is None else power + p
                nbuf[b + e, two(q)] = half.astype(bf16).reshape(2, T, N)
        pa[z, q] = power_row(power)
        for k in ZORD:
            back_copy(q, k, ya, o_recv).start()
            pa_copy(q, k).start()
        ya[mine(q)] = nbuf[z, two(q)]
        return carry

    w_wait(0)
    for k in range(1, 4):
        src = (z + k) % 4
        remote(bbuf.at[src], bbuf.at[src], b_send.at[0], b_recv.at[src], d, src).wait_recv()
    lax.fori_loop(0, LATE, mix_step, 0)

    def second_arrive(k, carry):
        arrive(k, True)
        return carry

    lax.fori_loop(1, 32, second_arrive, 0)

    def halo_b(s, slot):
        power = []
        for tt in range(2):
            t = s * 2 + tt
            total = acc[t_rows(t), 0:N] + tile_sum(slot, tt, hidx, hcnt, d * 4, t, recv2)
            act = jnp.maximum(total + bbuf[z][:, N : 2 * N].astype(f32), 0.0)
            acc[t_rows(t), 0:N] = act
            power.append(act * act)
        pb[z, s] = power_row(jnp.concatenate(power, axis=0))

    stream(hval, in_order, halo_b)

    def pb_copy(k):
        return remote(pb.at[z], pb.at[z], pb_send.at[k - 1], pb_recv.at[z], d, (z + k) % 4)

    for k in range(1, 4):
        pb_copy(k).start()
    lax.fori_loop(LATE, 8, mix_step, 0)
    for k in range(1, 4):
        src = (z + k) % 4
        remote(pb.at[src], pb.at[src], pb_send.at[0], pb_recv.at[src], d, src).wait_recv()

    part[...] = jnp.zeros_like(part)

    def norm_step(q, carry):
        for k in range(1, 4):
            src = (z + k) % 4
            back_wait(q, src, ya, o_recv)
            remote(pa.at[src, q], pa.at[src, q], pa_send.at[0], pa_recv.at[q * 4 + src], d, src).wait_recv()
        sums = [[None, None], [None, None]]
        for p in range(4):
            chunk = p * 8 + q
            power = pa[p, q] + pb[0, chunk] + pb[1, chunk] + pb[2, chunk] + pb[3, chunk]
            scale = jnp.broadcast_to(lax.rsqrt(power * (1.0 / 1024.0) + epsilon), (128, 256)).T
            at = pl.ds(p * 16 + q * 2, 2)
            acts = (
                ya[at].reshape(256, N).astype(f32),
                acc[pl.ds(pl.multiple_of(chunk * 256, 256), 256), 0:N],
            )
            for h in range(2):
                scaled = acts[h] * scale
                out[at, :, h * N : (h + 1) * N] = scaled.astype(bf16).reshape(2, T, N)
                for e, v in enumerate((scaled, scaled * scaled)):
                    v = jnp.sum(v, axis=0, keepdims=True)
                    sums[h][e] = v if sums[h][e] is None else sums[h][e] + v
        for h in range(2):
            for e in range(2):
                part[e : e + 1, h * N : (h + 1) * N] += sums[h][e]
        return carry

    lax.fori_loop(0, 8, norm_step, 0)

    def s1_copy(k):
        return remote(s1.at[d], s1.at[d], s1_send.at[k], s1_recv.at[d], (d + k) % 32, z)

    s1[d] = part[...]

    def s1_start(k, carry):
        s1_copy(k).start()
        return carry

    lax.fori_loop(1, 32, s1_start, 0)

    def last_mid(i, carry):
        mid_copy(i, True).wait_send()
        for cc in range(2):
            fwd_copy(i, cc, True).wait_send()
        return carry

    lax.fori_loop(0, 18, last_mid, 0)

    def last_dir(i, carry):
        dir_copy(i, True).wait_send()
        return carry

    lax.fori_loop(0, 26, last_dir, 0)

    def last_z(s, carry):
        z_copy(s // 3, s % 3, z_recv2).wait_send()
        return carry

    lax.fori_loop(0, 24, last_z, 0)

    def last_back(q, carry):
        for k in range(1, 4):
            back_copy(q, k, ya, o_recv).wait_send()
            pa_copy(q, k).wait_send()
        return carry

    lax.fori_loop(0, 8, last_back, 0)
    for k in range(1, 4):
        for h in range(2):
            w_copy(k, h).wait_send()
            w_give(k, h).wait_send()
        bias_copy(k).wait_send()
        pb_copy(k).wait_send()

    def s1_wait(k, carry):
        src = (d + k) % 32
        remote(s1.at[src], s1.at[src], s1_send.at[0], s1_recv.at[src], d, z).wait_recv()
        s1_copy(k).wait_send()
        return carry

    lax.fori_loop(1, 32, s1_wait, 0)
    sums = jnp.sum(s1[...], axis=0) * (1.0 / 262144.0)
    mean = sums[0:1, :]
    stats[0:1, :] = mean
    stats[1:2, :] = sums[1:2, :] - mean * mean


def on_device(
    features, weight, out_bias, local_index, local_count, local_vals,
    halo_index, halo_count, halo_vals, send_rows, send_count,
):
    smem = pl.BlockSpec(memory_space=pltpu.SMEM)
    hbm = pl.BlockSpec(memory_space=pl.ANY)
    bf16, f32 = jnp.bfloat16, jnp.float32
    V = pltpu.VMEM
    dma = lambda n: pltpu.SemaphoreType.DMA((n,))
    out, stats = pl.pallas_call(
        layer,
        out_shape=(V((64, T, 256), bf16), V((2, 256), f32)),
        in_specs=[hbm] + [smem] * 5 + [hbm] * 5,
        out_specs=(pl.BlockSpec(memory_space=V), pl.BlockSpec(memory_space=V)),
        scratch_shapes=[
            pltpu.SMEM((16384,), jnp.int32),
            V((65, T, 256), bf16),
            V((8192, 2, 128), bf16),
            V((HALF, 2, 128), bf16),
            V((72 + 26 * 2, T, 256), bf16),
            V((72, T, 256), bf16),
            V((72, T, N), bf16),
            V((128, T, 256), bf16),
            V((128, T, N), bf16),
            V((8192, 256), f32),
            V((SLOTS, 2, 4, 128, 128), bf16),
            V((4, 16, T, 256), bf16),
            V((4, 1024, 256), bf16),
            V((4, 1, 256), bf16),
            V((256,), bf16),
            V((4, 16, T, N), bf16),
            V((65, T, N), bf16),
            V((64, T, N), bf16),
            V((4, 8, 1, 256), f32),
            V((4, 32, 1, 256), f32),
            V((2, 256), f32),
            V((32, 2, 256), f32),
            dma(12), dma(32), dma(SLOTS), dma(6), dma(8), dma(6), dma(8), dma(3), dma(4),
            dma(18), dma(18), dma(18), dma(26), dma(36), dma(64), dma(64),
            dma(24), dma(32), dma(32), dma(24), dma(32), dma(32), dma(24), dma(32), dma(3), dma(4),
            dma(32), dma(32),
        ],
        compiler_params=pltpu.CompilerParams(
            collective_id=0, has_side_effects=True, vmem_limit_bytes=62000000
        ),
        name="layer",
    )(
        send_rows[0], send_count, local_index[0].T, local_count, halo_index[0].T, halo_count,
        features.reshape(64, T, 256), weight, out_bias, local_vals[0], halo_vals[0],
    )
    return out.reshape(8192, 256), stats


def solution(mesh):
    in_specs = (
        P("dom", "col"), P(None, "col"), P("col"),
        P("dom", None, None), P("dom", None), P("dom", None, None, None, None),
        P("dom", None, None), P("dom", None), P("dom", None, None, None, None),
        P("dom", None, None), P("dom", None),
    )
    return jax.shard_map(
        on_device, mesh=mesh, in_specs=in_specs,
        out_specs=(P("dom", "col"), P(None, "col")), check_vma=False,
    )
```

```python
import jax
import jax.numpy as jnp
from jax import lax
from jax.experimental import pallas as pl
from jax.experimental.pallas import tpu as pltpu
from jax.sharding import PartitionSpec as P

MESH = pl.DeviceIdType.MESH
epsilon = 1e-06

T = 128
HALF = 256
G = 64
ZORD = (2, 1, 3)
LATE = 6
SPLIT = 12
SMALL = 2.0**-8
TOP = 1e38
SLOTS = 4
N = 128


def dom_of(y, x, c):
    return (y * 4 + x) * 2 + c


def layer(
    sidx_hbm, scnt, lidx, lcnt, hidx, hcnt, feat_hbm, w_hbm, bias_hbm, lval, hval,
    out, stats,
    sidx, feat, tab, stage, send, mid, mid2, recv, recv2, acc, abuf, zrecv, wbuf, bbuf, b_own, nbuf,
    zb, ya, pa, pb, part, s1,
    in_sem, idx_sem, a_sem, w_send, w_recv, wg_send, wg_recv, b_send, b_recv,
    mid_send, mid_recv, mid_recv2, dir_send, fwd_send, fin_recv, fin_recv2,
    z_send, z_recv, z_recv2, n_send, zb_recv, o_recv, pa_send, pa_recv, pb_send, pb_recv,
    s1_send, s1_recv,
):
    f32, bf16 = jnp.float32, jnp.bfloat16
    d = lax.axis_index("dom")
    z = lax.axis_index("col")
    y, x, c = d // 8, (d // 2) % 4, d % 2

    def place(r, du, dv):
        dy = jnp.where(r == 0, dv, du)
        dx = jnp.where(r == 0, du, dv)
        return (y + dy) % 4, (x + dx) % 4

    def remote(src, dst, ssem, rsem, dom, col):
        return pltpu.make_async_remote_copy(
            src_ref=src, dst_ref=dst, send_sem=ssem, recv_sem=rsem,
            device_id={"dom": dom, "col": col}, device_id_type=MESH,
        )

    def feat_in(i):
        tiles = pl.ds(i * 8, 8)
        return pltpu.make_async_copy(feat_hbm.at[tiles], feat.at[tiles], in_sem.at[4 + i])

    for i in range(8):
        feat_in(i).start()

    def idx_in(p):
        return pltpu.make_async_copy(sidx_hbm.at[p], sidx.at[pl.ds(p * 512, 512)], idx_sem.at[p])

    for p in range(32):
        idx_in(p).start()
    w_in = pltpu.make_async_copy(w_hbm, wbuf.at[z], in_sem.at[1])
    w_in.start()
    b_in = pltpu.make_async_copy(bias_hbm, b_own, in_sem.at[2])
    b_in.start()

    def a_chunk(vals, chunk, slot):
        return pltpu.make_async_copy(vals.at[pl.ds(chunk * 2, 2)], abuf.at[slot], a_sem.at[slot])

    for s in range(SLOTS):
        a_chunk(lval, s, s).start()

    barrier = pltpu.get_barrier_semaphore()
    peers = [((d + k) % 32, z) for k in range(1, 32)] + [(d, (z + k) % 4) for k in range(1, 4)]
    for dom, col in peers:
        pl.semaphore_signal(
            barrier, inc=1, device_id={"dom": dom, "col": col}, device_id_type=MESH
        )


    row = lax.broadcasted_iota(jnp.int32, (256, 256), 0)
    lane = lax.broadcasted_iota(jnp.int32, (256, 256), 1)
    merge = jnp.where(row == 2 * (lane % 128) + lane // 128, 1.0, 0.0).astype(bf16)
    srow = lax.broadcasted_iota(jnp.int32, (2 * G, 2 * G), 0)
    slane = lax.broadcasted_iota(jnp.int32, (2 * G, 2 * G), 1)
    split = jnp.where(slane == 2 * (srow % G) + srow // G, 1.0, 0.0).astype(bf16)
    row_id = lax.broadcasted_iota(jnp.int32, (G, 128), 0)
    lane_id = lax.broadcasted_iota(jnp.int32, (G, 128), 1)

    feat[64] = jnp.zeros((T, 256), bf16)
    zb[64] = jnp.zeros((T, N), bf16)
    def build(i, carry):
        feat_in(i).wait()
        mixed = []
        for u in range(0, 8, 2):
            rows = [feat[i * 8 + u + e] for e in range(2)]
            both = jnp.concatenate(
                [
                    jnp.concatenate([rows[0][:, :128], rows[1][:, :128]], axis=1),
                    jnp.concatenate([rows[0][:, 128:], rows[1][:, 128:]], axis=1),
                ],
                axis=0,
            )
            mixed.append(jnp.dot(merge, both, preferred_element_type=f32).astype(bf16))
        for u in range(8):
            half = mixed[u // 2][:, u % 2 * 128 : (u % 2 + 1) * 128]
            tab[pl.ds(pl.multiple_of(i * 1024 + u * T, T), T)] = half.reshape(T, 2, 128)
        return carry

    lax.fori_loop(0, 8, build, 0)
    w_in.wait()
    b_in.wait()
    bbuf[z] = b_own[...].reshape(1, 256)
    for p in range(32):
        idx_in(p).wait()
    pl.semaphore_wait(barrier, len(peers))

    other = dom_of(y, x, 1 - c)

    def w_part(plane, h, core):
        return wbuf.at[plane, pl.ds(core * 512, 512), pl.ds(h * N, N)]

    def w_copy(k, h):
        part = w_part(z, h, c)
        return remote(part, part, w_send.at[h * 3 + k - 1], w_recv.at[h * 4 + z], d, (z + k) % 4)

    def w_give(k, h):
        src = (z + k) % 4
        part = w_part(src, h, c)
        return remote(part, part, wg_send.at[h * 3 + k - 1], wg_recv.at[h * 4 + src], other, z)

    def bias_copy(k):
        return remote(bbuf.at[z], bbuf.at[z], b_send.at[k - 1], b_recv.at[z], d, (z + k) % 4)

    def w_wait(h):
        for k in range(1, 4):
            src = (z + k) % 4
            part = w_part(src, h, c)
            remote(part, part, w_send.at[0], w_recv.at[h * 4 + src], d, src).wait_recv()
            w_give(k, h).start()
        for k in range(1, 4):
            src = (z + k) % 4
            part = w_part(src, h, 1 - c)
            remote(part, part, wg_send.at[0], wg_recv.at[h * 4 + src], d, z).wait_recv()

    for k in range(1, 4):
        w_copy(k, 1).start()

    def z_plane(o):
        far = jnp.where(o == 0, ZORD[0], jnp.where(o == 1, ZORD[1], jnp.where(o == 2, ZORD[2], 0)))
        return (z + far) % 4

    def z_copy(q, o, sems):
        plane = z_plane(o)
        return remote(
            feat.at[pl.ds(plane * 16 + q * 2, 2)], zrecv.at[z, pl.ds(q * 2, 2)],
            z_send.at[q * 3 + o], sems.at[q * 4 + z], d, plane,
        )

    def z_first(s, carry):
        z_copy(s // 3, s % 3, z_recv).start()
        return carry

    lax.fori_loop(0, 24, z_first, 0)

    def gather(dest, r, at, narrow):
        used = scnt[0, dest] - r * HALF
        base = dest * 512 + r * HALF
        for g in range(HALF // G):
            for u in range(G):
                stage[g * G + u] = tab[sidx[base + (g * G + u)]]
            both = stage[pl.ds(g * G, G)].reshape(2 * G, 128)
            parts = jnp.dot(split, both, preferred_element_type=f32)
            keep = row_id < used - g * G
            rows = pl.ds(g * G % T, G)
            if narrow:
                whole = jnp.where(lane_id < 64, parts[:G], pltpu.roll(parts[G:], 64, 1))
                send[at + g * G // T, rows, 0:128] = jnp.where(keep, whole, 0.0).astype(bf16)
            else:
                for h in range(2):
                    half = jnp.where(keep, parts[h * G : (h + 1) * G], 0.0)
                    send[at + g * G // T, rows, h * 128 : (h + 1) * 128] = half.astype(bf16)

    def mid_of(i):
        r = i % 2
        j = i // 2
        return r, 1 + (j + 1) % 3, 1 + j // 3

    def sent(at, n, narrow):
        return send.at[pl.ds(at, n), :, pl.ds(0, 128)] if narrow else send.at[pl.ds(at, n)]

    def mid_copy(i, narrow):
        r, du, dv = mid_of(i)
        ty, tx = place(r, du, 0)
        buf, sems = (mid2, mid_recv2) if narrow else (mid, mid_recv)
        return remote(
            sent(i * 4, 4, narrow), buf.at[pl.ds(i * 4, 4)], mid_send.at[i], sems.at[i],
            dom_of(ty, tx, c), z,
        )

    def mid_step(i, narrow):
        r, du, dv = mid_of(i)
        ty, tx = place(r, du, dv)

        def core(cc, carry):
            gather(dom_of(ty, tx, (c + cc) % 2), r, i * 4 + cc * 2, narrow)
            return carry

        lax.fori_loop(0, 2, core, 0)
        mid_copy(i, narrow).start()

    def dir_of(i):
        r = i % 2
        j = i // 2
        g = j // 6
        k = 1 + (j % 6) // 2
        cc = jnp.where(g == 2, 1, j % 2)
        du = jnp.where(g == 0, k, 0)
        dv = jnp.where(g == 1, k, 0)
        ty, tx = place(r, du, dv)
        return r, dom_of(ty, tx, (c + cc) % 2)

    def fin_at(src, r, narrow):
        buf, sems = (recv2, fin_recv2) if narrow else (recv, fin_recv)
        return buf.at[pl.ds(src * 4 + r * 2, 2)], sems.at[r * 32 + src]

    def dir_copy(i, narrow):
        r, dest = dir_of(i)
        dst, sem = fin_at(d, r, narrow)
        return remote(sent(72 + i * 2, 2, narrow), dst, dir_send.at[i], sem, dest, z)

    def fwd_copy(i, cc, narrow):
        r, du, dv = mid_of(i)
        ty, tx = place(r, 0, dv)
        sy, sx = place(r, 4 - du, 0)
        dst, sem = fin_at(dom_of(sy, sx, c), r, narrow)
        buf = mid2 if narrow else mid
        return remote(
            buf.at[pl.ds(i * 4 + cc * 2, 2)], dst, fwd_send.at[i * 2 + cc], sem,
            dom_of(ty, tx, (c + cc) % 2), z,
        )

    def dir_step(i, narrow):
        r, dest = dir_of(i)
        gather(dest, r, 72 + i * 2, narrow)
        dir_copy(i, narrow).start()

        @pl.when(i < 18)
        def _():
            mid_copy(i, narrow).wait_recv()
            for cc in range(2):
                fwd_copy(i, cc, narrow).start()

    def first_mid(i, carry):
        mid_step(i, False)
        return carry

    lax.fori_loop(0, 18, first_mid, 0)

    def two(q):
        return pl.ds(q * 2, 2)

    def mine(q):
        return pl.ds(z * 16 + q * 2, 2)

    def z_wait(q, src, sems):
        remote(
            feat.at[pl.ds(0, 2)], zrecv.at[src, two(q)], z_send.at[0],
            sems.at[q * 4 + src], d, src,
        ).wait_recv()

    def mix(q, sems, col, scale=None):
        zrecv[z, two(q)] = feat[mine(q)]
        for k in range(1, 4):
            z_wait(q, (z + k) % 4, sems)
        lhs = [zrecv[s, two(q)].reshape(256, 256) for s in range(4)]
        res = []
        for b in (0, 2):
            total = None
            for s in range(4):
                w = [wbuf[b + e, s * 256 : (s + 1) * 256, col : col + N] for e in range(2)]
                w = jnp.concatenate(w, axis=1)
                if scale is not None:
                    w = w * jnp.asarray(scale, bf16)
                p = jnp.dot(lhs[s], w, preferred_element_type=f32)
                total = p if total is None else total + p
            res.append(total)
        return res

    def back_copy(q, k, buf, sems):
        dst = (z + k) % 4
        return remote(
            nbuf.at[dst, two(q)], buf.at[mine(q)], n_send.at[q * 3 + k - 1],
            sems.at[q * 4 + z], d, dst,
        )

    def back_wait(q, src, buf, sems):
        remote(
            nbuf.at[0, two(q)], buf.at[pl.ds(src * 16 + q * 2, 2)], n_send.at[0],
            sems.at[q * 4 + src], d, src,
        ).wait_recv()

    def premix_step(q, carry):
        res = mix(q, z_recv, N, SMALL)
        for b in range(4):
            half = res[b // 2][:, (b % 2) * N : (b % 2 + 1) * N]
            nbuf[b, two(q)] = half.astype(bf16).reshape(2, T, N)
        for k in ZORD:
            back_copy(q, k, zb, zb_recv).start()
        zb[mine(q)] = nbuf[z, two(q)]
        return carry

    def first_dir(i, carry):
        dir_step(i, False)

        @pl.when(i % 5 == 4)
        def _():
            premix_step(i // 5, 0)

        return carry

    lax.fori_loop(0, 3, first_dir, 0)
    w_wait(1)
    lax.fori_loop(3, 26, first_dir, 0)
    lax.fori_loop(5, 6, premix_step, 0)

    def tile_sum(slot, tt, idx, cnt, zero, t, buf):
        total = None
        at = [jnp.where(k < cnt[0, t], idx[k, t], zero) for k in range(4)]
        for k in (0, 2):
            lhs = jnp.concatenate([abuf[slot, tt, k], abuf[slot, tt, k + 1]], axis=1)
            rhs = jnp.concatenate([buf[at[k]], buf[at[k + 1]]], axis=0)
            p = jnp.dot(lhs, rhs, preferred_element_type=f32)
            total = p if total is None else total + p
        return total

    def stream(vals, chunk_of, use):
        def step(s, carry):
            slot = s % SLOTS
            a_chunk(vals, chunk_of(s), slot).wait()
            use(s, slot)

            @pl.when(s + SLOTS < 32)
            def _():
                a_chunk(vals, chunk_of(s + SLOTS), slot).start()

            return carry

        lax.fori_loop(0, 32, step, 0)

    def ahead(vals, chunk_of):
        for s in range(SLOTS):
            a_chunk(vals, chunk_of(s), s).start()

    def t_rows(t):
        return pl.ds(pl.multiple_of(t * T, T), T)

    def in_order(s):
        return s

    def own_a(s, slot):
        for tt in range(2):
            t = s * 2 + tt
            acc[t_rows(t), :] = tile_sum(slot, tt, lidx, lcnt, 64, t, feat)

    stream(lval, in_order, own_a)
    lax.fori_loop(6, 8, premix_step, 0)
    for k in range(1, 4):
        w_copy(k, 0).start()
        bias_copy(k).start()

    def halo_chunk(s):
        return z_plane(s % 4) * 8 + s // 4

    ahead(hval, halo_chunk)

    def zb_wait(q, carry):
        for k in range(1, 4):
            back_wait(q, (z + k) % 4, zb, zb_recv)
        return carry

    lax.fori_loop(0, 8, zb_wait, 0)

    def rebuild(i, carry):
        mixed = []
        for u in range(0, 8, 2):
            rows = jnp.concatenate([zb[i * 8 + u], zb[i * 8 + u + 1]], axis=1)
            turned = [pltpu.roll(zb[i * 8 + u + e].astype(f32), 64, 1).astype(bf16) for e in range(2)]
            both = jnp.concatenate([rows, jnp.concatenate(turned, axis=1)], axis=0)
            mixed.append(jnp.dot(merge, both, preferred_element_type=f32).astype(bf16))
        for u in range(8):
            half = mixed[u // 2][:, u % 2 * 128 : (u % 2 + 1) * 128]
            tab[pl.ds(pl.multiple_of(i * 1024 + u * T, T), T)] = half.reshape(T, 2, 128)
        return carry

    lax.fori_loop(0, 8, rebuild, 0)

    def second_mid(i, carry):
        mid_copy(i, False).wait_send()
        mid_step(i, True)
        return carry

    lax.fori_loop(0, SPLIT, second_mid, 0)

    recv[pl.ds(d * 4, 4)] = jnp.zeros((4, T, 256), bf16)
    recv2[pl.ds(d * 4, 4)] = jnp.zeros((4, T, N), bf16)

    def z_sent(s, carry):
        z_copy(s // 3, s % 3, z_recv).wait_send()
        return carry

    lax.fori_loop(0, 24, z_sent, 0)

    def arrive(k, narrow):
        src = (d + k) % 32
        for r in range(2):
            dst, sem = fin_at(src, r, narrow)
            remote(sent(0, 2, narrow), dst, dir_send.at[0], sem, d, z).wait_recv()

    def first_arrive(k, carry):
        arrive(k, False)
        return carry

    lax.fori_loop(1, 32, first_arrive, 0)

    def halo_a(s, slot):
        chunk = halo_chunk(s)
        for tt in range(2):
            t = chunk * 2 + tt
            total = acc[t_rows(t), :] + tile_sum(slot, tt, hidx, hcnt, d * 4, t, recv)
            feat[t] = total.astype(bf16)

        @pl.when(s % 4 < 3)
        def _():
            z_copy(s // 4, s % 4, z_recv2).start()

    stream(hval, halo_chunk, halo_a)
    ahead(lval, in_order)

    lax.fori_loop(SPLIT, 18, second_mid, 0)

    def first_sent(i, carry):
        for cc in range(2):
            fwd_copy(i, cc, False).wait_send()
        return carry

    lax.fori_loop(0, 18, first_sent, 0)

    def second_dir(i, carry):
        dir_copy(i, False).wait_send()
        dir_step(i, True)
        return carry

    lax.fori_loop(0, 26, second_dir, 0)

    def own_b(s, slot):
        for tt in range(2):
            t = s * 2 + tt
            acc[t_rows(t), 0:N] = tile_sum(slot, tt, lidx, lcnt, 64, t, zb)

    stream(lval, in_order, own_b)
    ahead(hval, in_order)

    def back_sent(q, carry):
        for k in range(1, 4):
            back_copy(q, k, zb, zb_recv).wait_send()
        return carry

    lax.fori_loop(0, 8, back_sent, 0)

    def power_row(square):
        return jnp.sum(square.T, axis=0, keepdims=True)

    def pa_copy(q, k):
        dst = (z + k) % 4
        return remote(
            pa.at[z, q], pa.at[z, q], pa_send.at[q * 3 + k - 1], pa_recv.at[q * 4 + z], d, dst
        )

    def mix_step(q, carry):
        res = mix(q, z_recv2, 0)
        power = None
        for b in (0, 2):
            bias = jnp.concatenate([bbuf[b], bbuf[b + 1]], axis=1)
            keep = jnp.concatenate([bias[:, 0:N], bias[:, 256 : 256 + N]], axis=1)
            act = jnp.clip(res[b // 2] + keep.astype(f32), 0.0, TOP)
            for e in range(2):
                half = act[:, e * N : (e + 1) * N]
                p = half * half
                power = p if power is None else power + p
                nbuf[b + e, two(q)] = half.astype(bf16).reshape(2, T, N)
        pa[z, q] = power_row(power)
        for k in ZORD:
            back_copy(q, k, ya, o_recv).start()
            pa_copy(q, k).start()
        ya[mine(q)] = nbuf[z, two(q)]
        return carry

    w_wait(0)
    for k in range(1, 4):
        src = (z + k) % 4
        remote(bbuf.at[src], bbuf.at[src], b_send.at[0], b_recv.at[src], d, src).wait_recv()
    lax.fori_loop(0, LATE, mix_step, 0)

    def second_arrive(k, carry):
        arrive(k, True)
        return carry

    lax.fori_loop(1, 32, second_arrive, 0)

    def halo_b(s, slot):
        power = []
        for tt in range(2):
            t = s * 2 + tt
            total = acc[t_rows(t), 0:N] + tile_sum(slot, tt, hidx, hcnt, d * 4, t, recv2)
            act = jnp.maximum(total * (1.0 / SMALL) + bbuf[z][:, N : 2 * N].astype(f32), 0.0)
            acc[t_rows(t), 0:N] = act
            power.append(act * act)
        pb[z, s] = power_row(jnp.concatenate(power, axis=0))

    stream(hval, in_order, halo_b)

    def pb_copy(k):
        return remote(pb.at[z], pb.at[z], pb_send.at[k - 1], pb_recv.at[z], d, (z + k) % 4)

    for k in range(1, 4):
        pb_copy(k).start()
    lax.fori_loop(LATE, 8, mix_step, 0)
    for k in range(1, 4):
        src = (z + k) % 4
        remote(pb.at[src], pb.at[src], pb_send.at[0], pb_recv.at[src], d, src).wait_recv()

    part[...] = jnp.zeros_like(part)

    def norm_step(q, carry):
        for k in range(1, 4):
            src = (z + k) % 4
            back_wait(q, src, ya, o_recv)
            remote(pa.at[src, q], pa.at[src, q], pa_send.at[0], pa_recv.at[q * 4 + src], d, src).wait_recv()
        sums = [[None, None], [None, None]]
        for p in range(4):
            chunk = p * 8 + q
            power = pa[p, q] + pb[0, chunk] + pb[1, chunk] + pb[2, chunk] + pb[3, chunk]
            scale = jnp.broadcast_to(lax.rsqrt(power * (1.0 / 1024.0) + epsilon), (128, 256)).T
            at = pl.ds(p * 16 + q * 2, 2)
            acts = (
                ya[at].reshape(256, N).astype(f32),
                acc[pl.ds(pl.multiple_of(chunk * 256, 256), 256), 0:N],
            )
            for h in range(2):
                scaled = acts[h] * scale
                out[at, :, h * N : (h + 1) * N] = scaled.astype(bf16).reshape(2, T, N)
                for e, v in enumerate((scaled, scaled * scaled)):
                    v = jnp.sum(v, axis=0, keepdims=True)
                    sums[h][e] = v if sums[h][e] is None else sums[h][e] + v
        for h in range(2):
            for e in range(2):
                part[e : e + 1, h * N : (h + 1) * N] += sums[h][e]
        return carry

    lax.fori_loop(0, 8, norm_step, 0)

    def s1_copy(k):
        return remote(s1.at[d], s1.at[d], s1_send.at[k], s1_recv.at[d], (d + k) % 32, z)

    s1[d] = part[...]

    def s1_start(k, carry):
        s1_copy(k).start()
        return carry

    lax.fori_loop(1, 32, s1_start, 0)

    def last_mid(i, carry):
        mid_copy(i, True).wait_send()
        for cc in range(2):
            fwd_copy(i, cc, True).wait_send()
        return carry

    lax.fori_loop(0, 18, last_mid, 0)

    def last_dir(i, carry):
        dir_copy(i, True).wait_send()
        return carry

    lax.fori_loop(0, 26, last_dir, 0)

    def last_z(s, carry):
        z_copy(s // 3, s % 3, z_recv2).wait_send()
        return carry

    lax.fori_loop(0, 24, last_z, 0)

    def last_back(q, carry):
        for k in range(1, 4):
            back_copy(q, k, ya, o_recv).wait_send()
            pa_copy(q, k).wait_send()
        return carry

    lax.fori_loop(0, 8, last_back, 0)
    for k in range(1, 4):
        for h in range(2):
            w_copy(k, h).wait_send()
            w_give(k, h).wait_send()
        bias_copy(k).wait_send()
        pb_copy(k).wait_send()

    def s1_wait(k, carry):
        src = (d + k) % 32
        remote(s1.at[src], s1.at[src], s1_send.at[0], s1_recv.at[src], d, z).wait_recv()
        s1_copy(k).wait_send()
        return carry

    lax.fori_loop(1, 32, s1_wait, 0)
    sums = jnp.sum(s1[...], axis=0) * (1.0 / 262144.0)
    mean = sums[0:1, :]
    stats[0:1, :] = mean
    stats[1:2, :] = sums[1:2, :] - mean * mean


def on_device(
    features, weight, out_bias, local_index, local_count, local_vals,
    halo_index, halo_count, halo_vals, send_rows, send_count,
):
    smem = pl.BlockSpec(memory_space=pltpu.SMEM)
    hbm = pl.BlockSpec(memory_space=pl.ANY)
    bf16, f32 = jnp.bfloat16, jnp.float32
    V = pltpu.VMEM
    dma = lambda n: pltpu.SemaphoreType.DMA((n,))
    out, stats = pl.pallas_call(
        layer,
        out_shape=(V((64, T, 256), bf16), V((2, 256), f32)),
        in_specs=[hbm] + [smem] * 5 + [hbm] * 5,
        out_specs=(pl.BlockSpec(memory_space=V), pl.BlockSpec(memory_space=V)),
        scratch_shapes=[
            pltpu.SMEM((16384,), jnp.int32),
            V((65, T, 256), bf16),
            V((8192, 2, 128), bf16),
            V((HALF, 2, 128), bf16),
            V((72 + 26 * 2, T, 256), bf16),
            V((72, T, 256), bf16),
            V((72, T, N), bf16),
            V((128, T, 256), bf16),
            V((128, T, N), bf16),
            V((8192, 256), f32),
            V((SLOTS, 2, 4, 128, 128), bf16),
            V((4, 16, T, 256), bf16),
            V((4, 1024, 256), bf16),
            V((4, 1, 256), bf16),
            V((256,), bf16),
            V((4, 16, T, N), bf16),
            V((65, T, N), bf16),
            V((64, T, N), bf16),
            V((4, 8, 1, 256), f32),
            V((4, 32, 1, 256), f32),
            V((2, 256), f32),
            V((32, 2, 256), f32),
            dma(12), dma(32), dma(SLOTS), dma(6), dma(8), dma(6), dma(8), dma(3), dma(4),
            dma(18), dma(18), dma(18), dma(26), dma(36), dma(64), dma(64),
            dma(24), dma(32), dma(32), dma(24), dma(32), dma(32), dma(24), dma(32), dma(3), dma(4),
            dma(32), dma(32),
        ],
        compiler_params=pltpu.CompilerParams(
            collective_id=0, has_side_effects=True, vmem_limit_bytes=62000000
        ),
        name="layer",
    )(
        send_rows[0], send_count, local_index[0].T, local_count, halo_index[0].T, halo_count,
        features.reshape(64, T, 256), weight, out_bias, local_vals[0], halo_vals[0],
    )
    return out.reshape(8192, 256), stats


def solution(mesh):
    in_specs = (
        P("dom", "col"), P(None, "col"), P("col"),
        P("dom", None, None), P("dom", None), P("dom", None, None, None, None),
        P("dom", None, None), P("dom", None), P("dom", None, None, None, None),
        P("dom", None, None), P("dom", None),
    )
    return jax.shard_map(
        on_device, mesh=mesh, in_specs=in_specs,
        out_specs=(P("dom", "col"), P(None, "col")), check_vma=False,
    )
```
